32 devices in a mesh: freq: 2 (over x), param: 4 (over y, core), sens: 4 (over z).
Axes of the slice: x: 2, y: 2, z: 4, core: 2. Of those that a mesh axis runs over, the one named last changes fastest.
Arguments:
- series: bfloat16 [8, 600, 52], P(None, 'sens', 'freq'), may hold values from -6 to 6
- kernel: bfloat16 [2, 32, 600, 4096], P(None, 'freq', 'sens', 'param'), may hold values from -0.1875 to 0.1875
- prior_spectrum: float32 [32], P('freq'), may hold values from 0.3 to 1.5
- prior_scale: float32 [4096], P('param'), may hold values from 0.5 to 2
Outputs:
- adjoint_map: float32 [52, 8, 4096], P('freq', 'sens', 'param')
The draws below stay inside these ranges and needn't reach their ends.
All inputs are finite; a program needn't handle non-finite values.
Results may differ from the reference program's by a relative error of at most 0.0047.
Values may be sent and summed in bfloat16 or wider, within the bound.
A program may use at most 64 MiB of HBM per device.

```python
import math
import jax
import jax.numpy as jnp
from jax import lax

SENSORS = 600
LEN = 840
NB = 32
NT = 52
NP = 4096
PROBES = 8


def level_of(rng, extent, pieces, smallest, high):
    def one(position, blocks):
        steps = jax.random.uniform(jax.random.fold_in(jax.random.fold_in(rng, 6), position), (blocks,), jnp.float32, smallest / len(pieces), high / len(pieces))
        return jnp.repeat(jnp.exp(steps), extent[position] // blocks).reshape((-1,) + (1,) * (len(extent) - position - 1))

    level = one(*pieces[0])
    for cut in pieces[1:]:
        level = level * one(*cut)
    return level


def noise(rng, extent, width, reach, cuts=(), kind=jnp.bfloat16):
    entries = jax.random.normal(rng, extent, jnp.float32) * width
    if len(cuts) > 0:
        entries = level_of(rng, extent, cuts, -0.22, 0.18) * entries
    return jnp.clip(entries, min=-reach, max=reach).astype(kind)


def setup_inputs(seed: int = 0) -> dict:
    key_of = jax.random.split(jax.random.key(seed), 5)
    series = noise(key_of[0], (PROBES, SENSORS, NT), 1.0, 6.0, ((1, 4), (2, 2)))
    kernel = noise(key_of[1], (2, NB, SENSORS, NP), (2 * SENSORS) ** -0.5, 0.1875, ((1, 2), (2, 4), (3, 4)))
    prior_spectrum = jnp.clip(jnp.exp(math.log(1.5) - 1.60943787 * jax.random.uniform(key_of[2], (NB,), jnp.float32) ** level_of(key_of[2], (NB,), ((0, 2),), -0.2, 0.2)), 0.3, 1.5)
    prior_scale = jnp.clip(jnp.exp(math.log(2.0) - 1.3862944 * jax.random.uniform(key_of[3], (NP,), jnp.float32) ** level_of(key_of[3], (NP,), ((0, 4),), -0.2, 0.2)), 0.5, 2.0)
    return {"series": series, "kernel": kernel, "prior_spectrum": prior_spectrum, "prior_scale": prior_scale}


def phase_tables(bin_count, time_count):
    bin_index = jnp.arange(bin_count, dtype=jnp.int32)
    time_index = jnp.arange(time_count, dtype=jnp.int32)
    product = time_index[:, None] * bin_index[None, :] % LEN
    phase_angle = product.astype(jnp.float32) * (2.0 * math.pi / LEN)
    return (jnp.cos(phase_angle), jnp.sin(phase_angle))

def reference(series, kernel, prior_spectrum, prior_scale):
    highest = lax.Precision.HIGHEST
    cosine, sine_part = phase_tables(NB, NT)
    flat_rows = series.astype(jnp.float32).reshape(PROBES * SENSORS, NT)
    norm_time = 1.0 / math.sqrt(NT)
    spec_re = (jnp.dot(flat_rows, cosine, precision=highest) * norm_time).astype(jnp.bfloat16)
    spec_im = (-jnp.dot(flat_rows, sine_part, precision=highest) * norm_time).astype(jnp.bfloat16)
    spec_re = spec_re.reshape(PROBES, SENSORS, NB).transpose(2, 1, 0)
    spec_im = spec_im.reshape(PROBES, SENSORS, NB).transpose(2, 1, 0)

    def one_bin(index):
        kern_re = kernel[0, index]
        kern_im = kernel[1, index]
        data_re = spec_re[index].T
        data_im = spec_im[index].T
        real_part = jnp.dot(data_re, kern_re, preferred_element_type=jnp.float32) + jnp.dot(data_im, kern_im, preferred_element_type=jnp.float32)
        imag_part = jnp.dot(data_im, kern_re, preferred_element_type=jnp.float32) - jnp.dot(data_re, kern_im, preferred_element_type=jnp.float32)
        return jnp.stack([real_part, imag_part])
    spectra = lax.map(one_bin, jnp.arange(NB, dtype=jnp.int32))
    weights = prior_spectrum / math.sqrt(NB)
    scaled_spec = spectra * weights[:, None, None, None]
    image_re = scaled_spec[:, 0].reshape(NB, PROBES * NP)
    image_im = scaled_spec[:, 1].reshape(NB, PROBES * NP)
    image_field = jnp.dot(cosine, image_re, precision=highest) - jnp.dot(sine_part, image_im, precision=highest)
    image_field = image_field.reshape(NT, PROBES, NP)
    weighted = image_field * prior_scale
    padded = jnp.pad(weighted, ((0, 0), (0, 0), (1, 1)))
    smooth = 0.5 * weighted + 0.25 * (padded[:, :, :-2] + padded[:, :, 2:])
    return smooth * prior_scale
```

```python
import functools
import math

import jax
import jax.numpy as jnp
import numpy as np
from jax import lax
from jax.experimental import pallas as pl
from jax.experimental.pallas import tpu as pltpu
from jax.sharding import PartitionSpec as P

LEN = 840
MESH = pl.DeviceIdType.MESH
BF16 = jnp.bfloat16
F32 = jnp.float32
RESIDUAL = 2.0**-26
STEP = 256


def split(table):
    table = table.astype(np.float32)
    high = table.astype(BF16)
    low = (table - high.astype(np.float32)).astype(BF16)
    return high, low


def phases(groups, bins_dev, time_dev):
    bins, times = groups * bins_dev, groups * time_dev
    angle = 2.0 * np.pi * ((np.arange(times)[:, None] * np.arange(bins)[None, :]) % LEN) / LEN
    both = np.stack([np.cos(angle), -np.sin(angle)], axis=1)
    both = both.reshape(times, 2, groups, bins_dev).transpose(2, 0, 1, 3)
    return both.reshape(groups, times, 2 * bins_dev)


def factor(table, multiple):
    left, size, right = np.linalg.svd(table, full_matrices=False)
    rank = size.size
    for r in range(1, size.size):
        if np.abs(table - (left[:, :r] * size[:r]) @ right[:r]).max() < RESIDUAL:
            rank = r
            break
    rank = min(-(-rank // multiple) * multiple, size.size)
    return left * size, right, rank


def with_probes(table, probes):
    full = np.einsum("...ij,qr->...iqjr", table, np.eye(probes))
    lead = table.shape[:-2]
    return full.reshape(lead + (table.shape[-2] * probes, table.shape[-1] * probes))


def series_tables(groups, bins_dev, time_dev, probes):
    comps = phases(groups, bins_dev, time_dev) / math.sqrt(groups * time_dev)
    blocks = comps.reshape(groups, groups, time_dev, 2 * bins_dev).transpose(0, 1, 3, 2)
    parts = [factor(block.reshape(-1, time_dev), 2) for block in blocks]
    rank = max(part[2] for part in parts)
    short = np.stack([right[:rank] for _, right, _ in parts])
    long = np.stack([left[:, :rank] for left, _, _ in parts])
    long = long.reshape(groups, groups, 2 * bins_dev, rank)
    own = np.stack([blocks[g, g] for g in range(groups)])
    tables = [np.stack(split(with_probes(t, probes)), axis=-3) for t in (short, long, own)]
    return tables, rank


def image_tables(groups, bins_dev, time_dev, keep):
    comps = phases(groups, bins_dev, time_dev)
    parts = [factor(comp, 8) for comp in comps]
    rank = max(part[2] for part in parts)
    outer = np.stack([left[:, :rank] for left, _, _ in parts])
    outer = outer.reshape(groups, groups, time_dev, rank).transpose(1, 2, 0, 3)
    outer = outer.reshape(groups, time_dev, groups * rank)
    full = np.einsum("gtj,qr->gtqjr", outer, np.eye(keep))
    full = full.reshape(groups, time_dev * keep, groups * rank * keep)
    image = np.concatenate(split(full), axis=-1)
    inner = np.stack([right[:rank] for _, right, _ in parts])
    inner = inner.reshape(groups, rank, 2, bins_dev).transpose(0, 2, 1, 3)
    inner = np.repeat(inner, keep, axis=2)
    return image, np.tile(inner, (1, 1, 1, STEP // bins_dev)).astype(np.float32), rank


def body(
    cfg,
    series_hbm,
    kernel_hbm,
    prior_hbm,
    scale_hbm,
    short_hbm,
    long_hbm,
    own_hbm,
    img_hbm,
    inner_hbm,
    out_ref,
    kbuf,
    rows,
    prior,
    scale,
    short,
    long,
    own,
    img_tab,
    inner,
    squeezed,
    arrived,
    spread,
    ebuf,
    left_mat,
    sbuf,
    rbuf,
    relay,
    joined,
    gath,
    edges,
    halo_left,
    halo_right,
    small_sem,
    k_sem,
    g_send,
    g_recv,
    z_send,
    z_recv,
    relay_send,
    relay_recv,
    x_send,
    x_recv,
    hl_send,
    hl_recv,
    hr_send,
    hr_recv,
):
    groups, params, senses, chunks, bins_dev, probes = cfg
    f = lax.axis_index("freq")
    k = lax.axis_index("param")
    s = lax.axis_index("sens")
    depth = kernel_hbm.shape[1]
    width = kbuf.shape[-1]
    keep = probes // senses
    edge = halo_left.shape[-1]
    each = gath.shape[2]
    order = [0, chunks - 1] + list(range(1, chunks - 1)) if chunks > 1 else [0]

    def freq_peer(d):
        return lax.rem(f + d, groups)

    def sens_peer(d):
        return lax.rem(s + d, senses)

    small = [
        pltpu.make_async_copy(series_hbm, rows, small_sem.at[0]),
        pltpu.make_async_copy(short_hbm, short, small_sem.at[1]),
        pltpu.make_async_copy(own_hbm.at[f], own, small_sem.at[2]),
        pltpu.make_async_copy(long_hbm.at[f], long, small_sem.at[3]),
        pltpu.make_async_copy(prior_hbm, prior, small_sem.at[4]),
        pltpu.make_async_copy(inner_hbm.at[f], inner, small_sem.at[5]),
        pltpu.make_async_copy(scale_hbm, scale, small_sem.at[6]),
        pltpu.make_async_copy(img_hbm.at[f], img_tab, small_sem.at[7]),
    ]
    for copy in small:
        copy.start()

    barrier = pltpu.get_barrier_semaphore()
    for d in range(1, groups):
        pl.semaphore_signal(
            barrier, inc=1, device_id={"freq": freq_peer(d)}, device_id_type=MESH
        )
    for d in range(1, senses):
        pl.semaphore_signal(
            barrier, inc=1, device_id={"sens": sens_peer(d)}, device_id_type=MESH
        )
    has_left = k > 0
    has_right = k < params - 1

    @pl.when(has_left)
    def _():
        for d in range(groups):
            pl.semaphore_signal(
                barrier,
                inc=1,
                device_id={"freq": freq_peer(d), "param": k - 1},
                device_id_type=MESH,
            )

    @pl.when(has_right)
    def _():
        for d in range(groups):
            pl.semaphore_signal(
                barrier,
                inc=1,
                device_id={"freq": freq_peer(d), "param": k + 1},
                device_id_type=MESH,
            )

    small[0].wait()
    small[1].wait()
    loads = [
        [
            pltpu.make_async_copy(
                kernel_hbm.at[part, :, pl.ds(c * width, width)],
                kbuf.at[c, part],
                k_sem.at[c, part],
            )
            for part in range(2)
        ]
        for c in range(chunks)
    ]
    for c in order:
        for copy in loads[c]:
            copy.start()

    series = rows[...]
    for d in range(1, groups):
        g = freq_peer(d)
        squeezed[g] = (
            jnp.dot(short[g, 0], series, preferred_element_type=F32)
            + jnp.dot(short[g, 1], series, preferred_element_type=F32)
        ).astype(BF16)

    peers = groups + senses - 2
    beside = jnp.where(has_left, groups, 0) + jnp.where(has_right, groups, 0)
    pl.semaphore_wait(barrier, peers + beside)

    def series_copy(target, slot):
        return pltpu.make_async_remote_copy(
            src_ref=squeezed.at[target],
            dst_ref=arrived.at[slot],
            send_sem=g_send.at[target],
            recv_sem=g_recv.at[slot],
            device_id={"freq": target},
            device_id_type=MESH,
        )

    for d in range(1, groups):
        series_copy(freq_peer(d), f).start()
    for copy in small[2:]:
        copy.wait()
    row = lax.broadcasted_iota(jnp.int32, spread.shape, 0)
    lane = lax.broadcasted_iota(jnp.int32, spread.shape, 1)
    spread[...] = jnp.where(lane // bins_dev == row, 1.0, 0.0).astype(BF16)
    norm = 1.0 / math.sqrt(bins_dev * groups)
    lane = lax.broadcasted_iota(jnp.int32, (8, STEP), 1) % bins_dev
    value = jnp.zeros((8, STEP), F32)
    for b in range(bins_dev):
        value = jnp.where(lane == b, prior[b] * norm, value)
    inner[...] = inner[...] * value[:1]
    spec = jnp.dot(own[0], series, preferred_element_type=F32) + jnp.dot(
        own[1], series, preferred_element_type=F32
    )
    for d in range(1, groups):
        g = freq_peer(d)
        series_copy(g, g).wait_recv()
        came = arrived[g]
        spec = (
            spec
            + jnp.dot(long[g, 0], came, preferred_element_type=F32)
            + jnp.dot(long[g, 1], came, preferred_element_type=F32)
        )
    spec = spec.astype(BF16)
    odd = lax.broadcasted_iota(jnp.int32, (8, STEP), 0) % keep
    comp = bins_dev * probes
    for n in range(spread.shape[1] // STEP):
        cut = slice(n * STEP, (n + 1) * STEP)
        full = jnp.dot(spec, spread[:, cut], preferred_element_type=F32)
        for q in range(2):
            chosen = full[q * comp : q * comp + probes]
            for b in range(1, bins_dev):
                at = q * comp + b * probes
                chosen = jnp.where(lane[:probes] == b, full[at : at + probes], chosen)
            ebuf[q, :, cut] = chosen
        for j in range(senses):
            pair_of = []
            for q in range(2):
                e = jnp.broadcast_to(ebuf[q, j * keep : j * keep + 1, cut], (8, STEP))
                for r in range(1, keep):
                    at = j * keep + r
                    e = jnp.where(odd == r, ebuf[q, at : at + 1, cut], e)
                pair_of.append(jnp.concatenate([e] * (each // 8), axis=0))
            re, im = pair_of
            left_mat[0, j * each : (j + 1) * each, cut] = (inner[0] * re + inner[1] * im).astype(BF16)
            left_mat[1, j * each : (j + 1) * each, cut] = (inner[0] * im - inner[1] * re).astype(BF16)

    def z_copy(target, slot, c):
        return pltpu.make_async_remote_copy(
            src_ref=sbuf.at[target, c],
            dst_ref=rbuf.at[slot, c],
            send_sem=z_send.at[target, c],
            recv_sem=z_recv.at[slot, c],
            device_id={"sens": target},
            device_id_type=MESH,
        )

    paired = senses == 4
    if paired:
        pair = s + 1 - 2 * lax.rem(s, 2)
        across = senses - 1 - s
        other = senses - 1 - pair
        outer = jnp.logical_or(s == 0, s == senses - 1)
        within = jnp.logical_not(outer)

        @pl.when(within)
        def _():
            rbuf[other] = jnp.zeros(rbuf.shape[1:], BF16)

    def relay_copy(c):
        return pltpu.make_async_remote_copy(
            src_ref=sbuf.at[other, c],
            dst_ref=relay.at[c],
            send_sem=relay_send.at[c],
            recv_sem=relay_recv.at[c],
            device_id={"sens": pair},
            device_id_type=MESH,
        )

    def joined_copy(c):
        return pltpu.make_async_remote_copy(
            src_ref=joined.at[c],
            dst_ref=rbuf.at[s, c],
            send_sem=z_send.at[across, c],
            recv_sem=z_recv.at[s, c],
            device_id={"sens": across},
            device_id_type=MESH,
        )

    def send_sums(c):
        if not paired:
            for d in range(1, senses):
                z_copy(sens_peer(d), s, c).start()
            return

        @pl.when(outer)
        def _():
            relay_copy(c).start()
            z_copy(across, s, c).start()
            z_copy(pair, s, c).start()

        @pl.when(within)
        def _():
            z_copy(other, s, c).start()
            z_copy(pair, s, c).start()

    def pass_on(c):
        if not paired:
            return

        @pl.when(within)
        def _():
            relay_copy(c).wait_recv()
            both = sbuf[across, c].astype(F32) + relay[c].astype(F32)
            joined[c] = both.astype(BF16)
            joined_copy(c).start()

    def collect(c):
        total = sbuf[s, c].astype(F32)
        if not paired:
            for d in range(1, senses):
                z_copy(sens_peer(d), sens_peer(d), c).wait_recv()
                total = total + rbuf[sens_peer(d), c].astype(F32)
            return total
        z_copy(pair, pair, c).wait_recv()

        @pl.when(outer)
        def _():
            z_copy(other, other, c).wait_recv()

        z_copy(across, across, c).wait_recv()
        for slot in (pair, other, across):
            total = total + rbuf[slot, c].astype(F32)
        return total

    def drain(c):
        if not paired:
            for d in range(1, senses):
                z_copy(sens_peer(d), s, c).wait_send()
            return

        @pl.when(outer)
        def _():
            relay_copy(c).wait_send()
            z_copy(across, s, c).wait_send()
            z_copy(pair, s, c).wait_send()

        @pl.when(within)
        def _():
            z_copy(other, s, c).wait_send()
            z_copy(pair, s, c).wait_send()
            joined_copy(c).wait_send()

    for c in order:
        total = jnp.zeros((senses * each, width), F32)
        for part in range(2):
            loads[c][part].wait()
            total = total + jnp.dot(
                left_mat[part, :, :depth], kbuf[c, part], preferred_element_type=F32
            )
        for j in range(senses):
            sbuf[j, c] = total[j * each : (j + 1) * each].astype(BF16)
        send_sums(c)

    def x_copy(target, slot, c):
        return pltpu.make_async_remote_copy(
            src_ref=gath.at[f, c],
            dst_ref=gath.at[slot, c],
            send_sem=x_send.at[target, c],
            recv_sem=x_recv.at[slot, c],
            device_id={"freq": target},
            device_id_type=MESH,
        )

    def to_left(target, slot):
        return pltpu.make_async_remote_copy(
            src_ref=edges.at[0],
            dst_ref=halo_right.at[slot],
            send_sem=hl_send.at[target],
            recv_sem=hr_recv.at[slot],
            device_id={"freq": target, "param": jnp.maximum(k - 1, 0)},
            device_id_type=MESH,
        )

    def to_right(target, slot):
        return pltpu.make_async_remote_copy(
            src_ref=edges.at[1],
            dst_ref=halo_left.at[slot],
            send_sem=hr_send.at[target],
            recv_sem=hl_recv.at[slot],
            device_id={"freq": target, "param": jnp.minimum(k + 1, params - 1)},
            device_id_type=MESH,
        )

    cols = chunks * width
    pass_on(order[0])
    for i, c in enumerate(order):
        if i + 1 < chunks:
            pass_on(order[i + 1])
        total = collect(c)
        gath[f, c] = total.astype(BF16)
        for d in range(1, groups):
            x_copy(freq_peer(d), f, c).start()
        if c == 0:
            edges[0] = (total[:, :edge] * scale[:, :edge]).astype(BF16)

            @pl.when(has_left)
            def _():
                for d in range(groups):
                    to_left(freq_peer(d), f).start()

        if c == chunks - 1:
            edges[1] = (total[:, width - edge :] * scale[:, cols - edge :]).astype(BF16)

            @pl.when(has_right)
            def _():
                for d in range(groups):
                    to_right(freq_peer(d), f).start()

    @pl.when(has_left)
    def _():
        for d in range(groups):
            to_right(freq_peer(d), freq_peer(d)).wait_recv()

    @pl.when(jnp.logical_not(has_left))
    def _():
        halo_left[...] = jnp.zeros_like(halo_left)

    @pl.when(has_right)
    def _():
        for d in range(groups):
            to_left(freq_peer(d), freq_peer(d)).wait_recv()

    @pl.when(jnp.logical_not(has_right))
    def _():
        halo_right[...] = jnp.zeros_like(halo_right)

    def image_of(stack):
        return jnp.dot(
            img_tab[...], jnp.concatenate(stack + stack, axis=0), preferred_element_type=F32
        )

    left = image_of([halo_left[g] for g in range(groups)])
    right = image_of([halo_right[g] for g in range(groups)])
    scaled = [None] * chunks
    for c in order:
        for d in range(1, groups):
            g = freq_peer(d)
            x_copy(g, g, c).wait_recv()
        lanes = scale[:, c * width : (c + 1) * width]
        scaled[c] = image_of([gath[g, c] for g in range(groups)]) * lanes

    for c in range(chunks):
        mid = scaled[c]
        before = scaled[c - 1][:, width - 1 :] if c > 0 else left[:, edge - 1 :]
        after = scaled[c + 1][:, :1] if c < chunks - 1 else right[:, :1]
        lower = jnp.concatenate([before, mid[:, :-1]], axis=1)
        upper = jnp.concatenate([mid[:, 1:], after], axis=1)
        lanes = scale[:, c * width : (c + 1) * width]
        out_ref[:, c * width : (c + 1) * width] = lanes * (0.5 * mid + 0.25 * (lower + upper))

    for d in range(1, groups):
        series_copy(freq_peer(d), f).wait_send()
        for c in range(chunks):
            x_copy(freq_peer(d), f, c).wait_send()
    for c in range(chunks):
        drain(c)

    @pl.when(has_left)
    def _():
        for d in range(groups):
            to_left(freq_peer(d), f).wait_send()

    @pl.when(has_right)
    def _():
        for d in range(groups):
            to_right(freq_peer(d), f).wait_send()


def local(mesh_shape, series, kernel, prior_spectrum, prior_scale):
    groups, params, senses = (mesh_shape[n] for n in ("freq", "param", "sens"))
    probes, sens_dev, time_dev = series.shape
    _, bins_dev, _, cols = kernel.shape
    keep = probes // senses
    chunks = 4
    width = cols // chunks
    edge = min(128, width)
    rows = time_dev * keep
    depth = sens_dev * bins_dev
    steps = -(-depth // STEP) * STEP
    (short, long, own), squeeze = series_tables(groups, bins_dev, time_dev, probes)
    img_tab, inner, rank = image_tables(groups, bins_dev, time_dev, keep)
    each = rank * keep
    dma = pltpu.SemaphoreType.DMA
    out = pl.pallas_call(
        functools.partial(body, (groups, params, senses, chunks, bins_dev, probes)),
        out_shape=jax.ShapeDtypeStruct((rows, cols), F32),
        in_specs=[pl.BlockSpec(memory_space=pltpu.HBM)] * 9,
        out_specs=pl.BlockSpec(memory_space=pltpu.VMEM),
        scratch_shapes=[
            pltpu.VMEM((chunks, 2, depth, width), BF16),
            pltpu.VMEM((time_dev * probes, sens_dev), BF16),
            pltpu.SMEM((bins_dev,), F32),
            pltpu.VMEM((1, cols), F32),
            pltpu.VMEM(short.shape, BF16),
            pltpu.VMEM(long.shape[1:], BF16),
            pltpu.VMEM(own.shape[1:], BF16),
            pltpu.VMEM(img_tab.shape[1:], BF16),
            pltpu.VMEM(inner.shape[1:], F32),
            pltpu.VMEM((groups, squeeze * probes, sens_dev), BF16),
            pltpu.VMEM((groups, squeeze * probes, sens_dev), BF16),
            pltpu.VMEM((sens_dev, steps), BF16),
            pltpu.VMEM((2, probes, steps), F32),
            pltpu.VMEM((2, senses * each, steps), BF16),
            pltpu.VMEM((senses, chunks, each, width), BF16),
            pltpu.VMEM((senses, chunks, each, width), BF16),
            pltpu.VMEM((chunks, each, width), BF16),
            pltpu.VMEM((chunks, each, width), BF16),
            pltpu.VMEM((groups, chunks, each, width), BF16),
            pltpu.VMEM((2, each, edge), BF16),
            pltpu.VMEM((groups, each, edge), BF16),
            pltpu.VMEM((groups, each, edge), BF16),
            dma((8,)),
            dma((chunks, 2)),
            dma((groups,)),
            dma((groups,)),
            dma((senses, chunks)),
            dma((senses, chunks)),
            dma((chunks,)),
            dma((chunks,)),
            dma((groups, chunks)),
            dma((groups, chunks)),
            dma((groups,)),
            dma((groups,)),
            dma((groups,)),
            dma((groups,)),
        ],
        compiler_params=pltpu.CompilerParams(
            collective_id=0, has_side_effects=True, vmem_limit_bytes=60 * 1024 * 1024
        ),
    )(
        series.transpose(2, 0, 1).reshape(time_dev * probes, sens_dev),
        kernel.transpose(0, 2, 1, 3).reshape(2, depth, cols),
        prior_spectrum,
        prior_scale.reshape(1, cols),
        jnp.asarray(short),
        jnp.asarray(long),
        jnp.asarray(own),
        jnp.asarray(img_tab),
        jnp.asarray(inner),
    )
    return out.reshape(time_dev, keep, cols)


def solution(mesh):
    placed = (P(None, "sens", "freq"), P(None, "freq", "sens", "param"), P("freq"), P("param"))
    return jax.shard_map(
        functools.partial(local, dict(mesh.shape)),
        mesh=mesh,
        in_specs=placed,
        out_specs=P("freq", "sens", "param"),
        check_vma=False,
    )
```

```python
import functools
import math

import jax
import jax.numpy as jnp
import numpy as np
from jax import lax
from jax.experimental import pallas as pl
from jax.experimental.pallas import tpu as pltpu
from jax.sharding import PartitionSpec as P

LEN = 840
MESH = pl.DeviceIdType.MESH
BF16 = jnp.bfloat16
F32 = jnp.float32
RESIDUAL = 2.0**-26
STEP = 256
LANES = 128


def split(table):
    table = table.astype(np.float32)
    high = table.astype(BF16)
    low = (table - high.astype(np.float32)).astype(BF16)
    return high, low


def phases(groups, bins_dev, time_dev):
    bins, times = groups * bins_dev, groups * time_dev
    angle = 2.0 * np.pi * ((np.arange(times)[:, None] * np.arange(bins)[None, :]) % LEN) / LEN
    both = np.stack([np.cos(angle), -np.sin(angle)], axis=1)
    both = both.reshape(times, 2, groups, bins_dev).transpose(2, 0, 1, 3)
    return both.reshape(groups, times, 2 * bins_dev)


def factor(table, multiple):
    left, size, right = np.linalg.svd(table, full_matrices=False)
    rank = size.size
    for r in range(1, size.size):
        if np.abs(table - (left[:, :r] * size[:r]) @ right[:r]).max() < RESIDUAL:
            rank = r
            break
    rank = min(-(-rank // multiple) * multiple, size.size)
    return left * size, right, rank


def with_probes(table, probes):
    full = np.einsum("...ij,qr->...iqjr", table, np.eye(probes))
    lead = table.shape[:-2]
    return full.reshape(lead + (table.shape[-2] * probes, table.shape[-1] * probes))


def series_tables(groups, bins_dev, time_dev, probes):
    comps = phases(groups, bins_dev, time_dev) / math.sqrt(groups * time_dev)
    blocks = comps.reshape(groups, groups, time_dev, 2 * bins_dev).transpose(0, 1, 3, 2)
    parts = [factor(block.reshape(-1, time_dev), 2) for block in blocks]
    rank = max(part[2] for part in parts)
    short = np.stack([right[:rank] for _, right, _ in parts])
    short = np.stack(split(with_probes(short, probes)), axis=1)
    long = np.stack([left[:, :rank] for left, _, _ in parts])
    long = long.reshape(groups, groups, 2, bins_dev, rank).transpose(0, 1, 2, 4, 3)
    long = np.stack([np.roll(long[g], -g, axis=0) for g in range(groups)])
    return short, long.reshape(groups, -1, bins_dev), rank


def image_tables(groups, bins_dev, time_dev, keep):
    comps = phases(groups, bins_dev, time_dev)
    parts = [factor(comp, 8) for comp in comps]
    rank = max(part[2] for part in parts)
    outer = np.stack([left[:, :rank] for left, _, _ in parts])
    outer = outer.reshape(groups, groups, time_dev, rank).transpose(1, 2, 0, 3)
    full = np.einsum("gthj,qr->gtqhjr", outer, np.eye(keep))
    full = full.reshape(groups, time_dev * keep, groups, rank * keep)
    own = np.stack([full[g, :, g] for g in range(groups)])
    high, low = split(full.reshape(groups, time_dev * keep, -1))
    image = np.concatenate([high, low, split(own)[0]], axis=-1)
    inner = np.stack([right[:rank] for _, right, _ in parts])
    inner = inner.reshape(groups, rank, 2, bins_dev).transpose(0, 2, 1, 3)
    return image, np.repeat(inner, keep, axis=2).reshape(groups, -1, bins_dev), rank


def body(
    cfg,
    series_hbm,
    kernel_hbm,
    prior_hbm,
    scale_hbm,
    short_hbm,
    tabs_hbm,
    img_hbm,
    out_ref,
    kbufs,
    rows,
    prior,
    scale,
    short,
    tabs,
    img_tab,
    inner,
    squeezed,
    arrived,
    spread,
    ebuf,
    left_mat,
    sbuf,
    rbuf,
    relay,
    joined,
    gath,
    lows,
    scaled,
    edges,
    halo_left,
    halo_right,
    small_sem,
    k_sem,
    g_send,
    g_recv,
    z_send,
    z_recv,
    relay_recv,
    x_send,
    x_recv,
    hl_send,
    hl_recv,
    hr_send,
    hr_recv,
    ready_x,
    ready_z,
    ready_far,
):
    groups, params, senses, chunks, direct, bins_dev, probes, squeeze = cfg
    f = lax.axis_index("freq")
    k = lax.axis_index("param")
    s = lax.axis_index("sens")
    sens_dev = rows.shape[1]
    depth = kernel_hbm.shape[1]
    padded = left_mat.shape[1] // 2
    keep = probes // senses
    each = gath.shape[2]
    cols = scale.shape[1]
    count = len(chunks)
    has_left = k > 0
    has_right = k < params - 1
    has_under = s > 0
    has_over = s < senses - 1
    outer = jnp.logical_or(s == 0, s == senses - 1)
    within = jnp.logical_not(outer)
    pair = s + 1 - 2 * lax.rem(s, 2)
    across = senses - 1 - s
    other = senses - 1 - pair

    def freq_peer(d):
        return lax.rem(f + d, groups)

    def tell(sem, **where):
        pl.semaphore_signal(sem, inc=1, device_id=where, device_id_type=MESH)

    small = [
        pltpu.make_async_copy(series_hbm, rows, small_sem.at[0]),
        pltpu.make_async_copy(short_hbm, short, small_sem.at[1]),
        pltpu.make_async_copy(tabs_hbm.at[f], tabs, small_sem.at[2]),
        pltpu.make_async_copy(prior_hbm, prior, small_sem.at[3]),
        pltpu.make_async_copy(scale_hbm, scale, small_sem.at[4]),
        pltpu.make_async_copy(img_hbm.at[f], img_tab, small_sem.at[5]),
    ]
    for copy in small:
        copy.start()

    barrier = pltpu.get_barrier_semaphore()
    for d in range(1, groups):
        tell(barrier, freq=freq_peer(d))

    @pl.when(has_under)
    def _():
        tell(barrier, sens=s - 1)

    @pl.when(has_over)
    def _():
        tell(barrier, sens=s + 1)

    @pl.when(has_left)
    def _():
        tell(barrier, param=k - 1)

    @pl.when(has_right)
    def _():
        tell(barrier, param=k + 1)

    row = lax.broadcasted_iota(jnp.int32, spread.shape, 0)
    lane = lax.broadcasted_iota(jnp.int32, spread.shape, 1)
    spread[...] = jnp.where(lane // bins_dev == row, 1.0, 0.0).astype(BF16)
    for buf in kbufs:
        pad = jnp.zeros((padded - depth, buf.shape[1]), BF16)
        buf[depth:padded] = pad
        buf[padded + depth :] = pad

    small[0].wait()
    small[1].wait()
    loads = [
        [
            pltpu.make_async_copy(
                kernel_hbm.at[part, :, pl.ds(at, width)],
                kbufs[c].at[pl.ds(part * padded, depth)],
                k_sem.at[c, part],
            )
            for part in range(2)
        ]
        for c, (at, width) in enumerate(chunks)
    ]
    for group in loads:
        for copy in group:
            copy.start()

    series = rows[...]

    def shortened(g):
        return jnp.dot(short[g, 0], series, preferred_element_type=F32) + jnp.dot(
            short[g, 1], series, preferred_element_type=F32
        )

    for d in range(1, groups):
        g = freq_peer(d)
        squeezed[g] = shortened(g).astype(BF16)

    beside = [has_under, has_over, has_left, has_right]
    pl.semaphore_wait(barrier, groups - 1 + sum(jnp.where(b, 1, 0) for b in beside))

    def series_copy(target, slot):
        return pltpu.make_async_remote_copy(
            src_ref=squeezed.at[target],
            dst_ref=arrived.at[slot],
            send_sem=g_send,
            recv_sem=g_recv,
            device_id={"freq": target},
            device_id_type=MESH,
        )

    for d in range(1, groups):
        series_copy(freq_peer(d), f).start()
    for d in range(1, groups):
        tell(ready_x, freq=freq_peer(d))

    @pl.when(within)
    def _():
        tell(ready_z, sens=s - 1)
        tell(ready_z, sens=s + 1)

    for copy in small[2:]:
        copy.wait()
    norm = 1.0 / math.sqrt(bins_dev * groups)
    lane = lax.broadcasted_iota(jnp.int32, (8, STEP), 1) % bins_dev
    value = jnp.zeros((8, STEP), F32)
    for b in range(bins_dev):
        value = jnp.where(lane == b, prior[b] * norm, value)
    base = groups * 2 * squeeze
    for q in range(2):
        inner[q] = tabs[base + q * each : base + (q + 1) * each] * value[:1]

    cuts = [(at, min(STEP, padded - at)) for at in range(0, padded, STEP)]

    def expand(coefs, at, width):
        first = at // bins_dev // LANES * LANES
        last = min(first + LANES, sens_dev)
        return jnp.dot(
            coefs[:, first:last], spread[first:last, at : at + width], preferred_element_type=F32
        )

    def weighed(full, d, q, width):
        total = None
        for j in range(squeeze):
            at = (d * 2 + q) * squeeze + j
            term = full[j * probes : (j + 1) * probes] * tabs[at : at + 1, :width]
            total = term if total is None else total + term
        return total

    mine = shortened(f)
    high = mine.astype(BF16)
    low = (mine - high.astype(F32)).astype(BF16)
    mine = jnp.concatenate([high, low], axis=0)
    for at, width in cuts:
        full = expand(mine, at, width)
        full = full[: squeeze * probes] + full[squeeze * probes :]
        for q in range(2):
            ebuf[q, :, at : at + width] = weighed(full, 0, q, width)

    pl.semaphore_wait(ready_z, 1)

    @pl.when(within)
    def _():
        tell(ready_far, sens=pair)

    for copy in loads[0]:
        copy.wait()

    def series_done():
        return pltpu.make_async_remote_copy(
            src_ref=squeezed.at[pl.ds(0, groups - 1)],
            dst_ref=arrived.at[pl.ds(0, groups - 1)],
            send_sem=g_send,
            recv_sem=g_recv,
            device_id={"freq": freq_peer(1)},
            device_id_type=MESH,
        )

    series_done().wait_recv()
    came = [arrived[freq_peer(d)] for d in range(1, groups)]
    for at, width in cuts:
        cut = slice(at, at + width)
        fulls = [expand(c, at, width) for c in came]
        for q in range(2):
            total = ebuf[q, :, cut]
            for d in range(1, groups):
                total = total + weighed(fulls[d - 1], d, q, width)
            ebuf[q, :, cut] = total
        which = lax.broadcasted_iota(jnp.int32, (8, width), 0) % keep
        for j in range(senses):
            both = []
            for q in range(2):
                e = jnp.broadcast_to(ebuf[q, j * keep : j * keep + 1, cut], (8, width))
                for r in range(1, keep):
                    here = j * keep + r
                    e = jnp.where(which == r, ebuf[q, here : here + 1, cut], e)
                both.append(jnp.concatenate([e] * (each // 8), axis=0))
            re, im = both
            one, two = inner[0, :, :width], inner[1, :, :width]
            block = slice(j * each, (j + 1) * each)
            left_mat[block, cut] = (one * re + two * im).astype(BF16)
            left_mat[block, padded + at : padded + at + width] = (one * im - two * re).astype(BF16)

    def blocks(c):
        at, width = chunks[c]
        return pl.ds(at // LANES, width // LANES)

    def remote(src, dst, send, recv, **where):
        return pltpu.make_async_remote_copy(
            src_ref=src,
            dst_ref=dst,
            send_sem=send,
            recv_sem=recv,
            device_id=where,
            device_id_type=MESH,
        )

    def z_copy(target, c):
        return remote(
            sbuf.at[target, blocks(c)], rbuf.at[s, blocks(c)], z_send, z_recv.at[c], sens=target
        )

    def z_done(units, c):
        part = rbuf.at[pl.ds(0, units), blocks(c)]
        return remote(part, part, z_send, z_recv.at[c], sens=pair)

    def relay_copy(c):
        return remote(
            sbuf.at[other, blocks(c)], relay.at[blocks(c)], z_send, relay_recv.at[c], sens=pair
        )

    def joined_copy(c):
        return remote(
            joined.at[blocks(c)], rbuf.at[s, blocks(c)], z_send, z_recv.at[c], sens=across
        )

    def send_sums(c):
        if c in direct:
            for target in (across, other, pair):
                z_copy(target, c).start()
            return

        @pl.when(outer)
        def _():
            relay_copy(c).start()
            z_copy(across, c).start()
            z_copy(pair, c).start()

        @pl.when(within)
        def _():
            z_copy(other, c).start()
            z_copy(pair, c).start()

    def pass_on(c):
        if c in direct:
            return

        @pl.when(within)
        def _():
            relay_copy(c).wait_recv()
            both = sbuf[across, blocks(c)].astype(F32) + relay[blocks(c)].astype(F32)
            joined[blocks(c)] = both.astype(BF16)
            joined_copy(c).start()

    def collect(c):
        if c in direct:
            z_done(3, c).wait_recv()
        else:

            @pl.when(outer)
            def _():
                z_done(3, c).wait_recv()

            @pl.when(within)
            def _():
                z_done(2, c).wait_recv()

        total = sbuf[s, blocks(c)].astype(F32)
        for slot in (pair, other, across):
            total = total + rbuf[slot, blocks(c)].astype(F32)
        return total

    @pl.when(within)
    def _():
        rbuf[other] = jnp.zeros(rbuf.shape[1:], BF16)

    for c, (at, width) in enumerate(chunks):
        if c > 0:
            for copy in loads[c]:
                copy.wait()
        total = jnp.dot(left_mat[...], kbufs[c][...], preferred_element_type=F32)
        total = total.astype(BF16)
        for j in range(senses):
            for b in range(width // LANES):
                sbuf[j, at // LANES + b] = total[
                    j * each : (j + 1) * each, b * LANES : (b + 1) * LANES
                ]
        if c == 0:

            @pl.when(outer)
            def _():
                pl.semaphore_wait(ready_far, 1)

        send_sums(c)

    def x_copy(target, c):
        part = gath.at[f, blocks(c)]
        return remote(part, part, x_send, x_recv.at[c], freq=target)

    def x_done(c):
        part = gath.at[pl.ds(0, groups - 1), blocks(c)]
        return remote(part, part, x_send, x_recv.at[c], freq=freq_peer(1))

    def to_left(target):
        return remote(
            edges.at[0],
            halo_right.at[f],
            hl_send,
            hr_recv,
            freq=target,
            param=jnp.maximum(k - 1, 0),
        )

    def to_right(target):
        return remote(
            edges.at[1],
            halo_left.at[f],
            hr_send,
            hl_recv,
            freq=target,
            param=jnp.minimum(k + 1, params - 1),
        )

    def image_of(stack, low):
        wide = 2 * groups * each
        full = jnp.concatenate(stack + stack + ([] if low is None else [low]), axis=0)
        table = img_tab[:, : wide if low is None else wide + each]
        return jnp.dot(table, full, preferred_element_type=F32)

    def across_lanes(parts):
        return parts[0] if len(parts) == 1 else jnp.concatenate(parts, axis=1)

    def finish(c):
        x_done(c).wait_recv()
        at, width = chunks[c]
        span = range(at // LANES, (at + width) // LANES)
        stack = [across_lanes([gath[g, b] for b in span]) for g in range(groups)]
        image = image_of(stack, across_lanes([lows[b] for b in span]))
        scaled[:, at : at + width] = image * scale[:, at : at + width]

    pl.semaphore_wait(ready_x, groups - 1)
    pass_on(0)
    for c, (at, width) in enumerate(chunks):
        if c + 1 < count:
            pass_on(c + 1)
        total = collect(c)
        high = total.astype(BF16)
        gath[f, blocks(c)] = high
        for d in range(1, groups):
            x_copy(freq_peer(d), c).start()
        lows[blocks(c)] = (total - high.astype(F32)).astype(BF16)
        if at == 0:
            edges[0] = (total[0] * scale[:, :LANES]).astype(BF16)

            @pl.when(has_left)
            def _():
                for d in range(groups):
                    to_left(freq_peer(d)).start()

        if at + width == cols:
            edges[1] = (total[width // LANES - 1] * scale[:, cols - LANES :]).astype(BF16)

            @pl.when(has_right)
            def _():
                for d in range(groups):
                    to_right(freq_peer(d)).start()

        if c >= 2:
            finish(c - 2)

    def halo_done(ref, send, recv):
        return remote(ref, ref, send, recv, freq=freq_peer(1))

    @pl.when(has_left)
    def _():
        halo_done(halo_left, hr_send, hl_recv).wait_recv()

    @pl.when(jnp.logical_not(has_left))
    def _():
        halo_left[...] = jnp.zeros_like(halo_left)

    @pl.when(has_right)
    def _():
        halo_done(halo_right, hl_send, hr_recv).wait_recv()

    @pl.when(jnp.logical_not(has_right))
    def _():
        halo_right[...] = jnp.zeros_like(halo_right)

    left = image_of([halo_left[g] for g in range(groups)], None)
    right = image_of([halo_right[g] for g in range(groups)], None)
    for c in range(max(count - 2, 0), count):
        finish(c)

    for at in range(0, cols, STEP):
        end = at + STEP
        mid = scaled[:, at:end]
        before = scaled[:, at - 1 : at] if at > 0 else left[:, LANES - 1 :]
        after = scaled[:, end : end + 1] if end < cols else right[:, :1]
        lower = jnp.concatenate([before, mid[:, :-1]], axis=1)
        upper = jnp.concatenate([mid[:, 1:], after], axis=1)
        value = scale[:, at:end] * (0.5 * mid + 0.25 * (lower + upper))
        out_ref[:, :, at:end] = value.reshape(out_ref.shape[0], keep, STEP)

    series_done().wait_send()
    part = sbuf.at[pl.ds(0, 3)]
    remote(part, part, z_send, z_recv.at[0], sens=pair).wait_send()
    part = gath.at[pl.ds(0, groups - 1)]
    remote(part, part, x_send, x_recv.at[0], freq=freq_peer(1)).wait_send()

    @pl.when(has_left)
    def _():
        halo_done(halo_right, hl_send, hr_recv).wait_send()

    @pl.when(has_right)
    def _():
        halo_done(halo_left, hr_send, hl_recv).wait_send()


def local(mesh_shape, series, kernel, prior_spectrum, prior_scale):
    groups, params, senses = (mesh_shape[n] for n in ("freq", "param", "sens"))
    assert senses == 4 and groups > 1
    probes, sens_dev, time_dev = series.shape
    _, bins_dev, _, cols = kernel.shape
    keep = probes // senses
    quarter = cols // 4
    chunks = [(0, quarter), (3 * quarter, quarter), (quarter, quarter), (2 * quarter, quarter)]
    direct = ()
    count = len(chunks)
    depth = sens_dev * bins_dev
    padded = -(-depth // LANES) * LANES
    short, long, squeeze = series_tables(groups, bins_dev, time_dev, probes)
    img_tab, inner, rank = image_tables(groups, bins_dev, time_dev, keep)
    tabs = np.concatenate([long, inner], axis=1)
    tabs = np.tile(tabs, (1, 1, STEP // bins_dev)).astype(np.float32)
    each = rank * keep
    spans = cols // LANES
    dma = pltpu.SemaphoreType.DMA
    plain = pltpu.SemaphoreType.REGULAR
    return pl.pallas_call(
        functools.partial(
            body, (groups, params, senses, chunks, direct, bins_dev, probes, squeeze)
        ),
        out_shape=pltpu.VMEM((time_dev, keep, cols), F32),
        in_specs=[pl.BlockSpec(memory_space=pltpu.HBM)] * 7,
        out_specs=pl.BlockSpec(memory_space=pltpu.VMEM),
        scratch_shapes=[
            [pltpu.VMEM((2 * padded, width), BF16) for _, width in chunks],
            pltpu.VMEM((time_dev * probes, sens_dev), BF16),
            pltpu.SMEM((bins_dev,), F32),
            pltpu.VMEM((1, cols), F32),
            pltpu.VMEM(short.shape, BF16),
            pltpu.VMEM(tabs.shape[1:], F32),
            pltpu.VMEM(img_tab.shape[1:], BF16),
            pltpu.VMEM((2, each, STEP), F32),
            pltpu.VMEM((groups, squeeze * probes, sens_dev), BF16),
            pltpu.VMEM((groups, squeeze * probes, sens_dev), BF16),
            pltpu.VMEM((sens_dev, padded), BF16),
            pltpu.VMEM((2, probes, padded), F32),
            pltpu.VMEM((senses * each, 2 * padded), BF16),
            pltpu.VMEM((senses, spans, each, LANES), BF16),
            pltpu.VMEM((senses, spans, each, LANES), BF16),
            pltpu.VMEM((spans, each, LANES), BF16),
            pltpu.VMEM((spans, each, LANES), BF16),
            pltpu.VMEM((groups, spans, each, LANES), BF16),
            pltpu.VMEM((spans, each, LANES), BF16),
            pltpu.VMEM((time_dev * keep, cols), F32),
            pltpu.VMEM((2, each, LANES), BF16),
            pltpu.VMEM((groups, each, LANES), BF16),
            pltpu.VMEM((groups, each, LANES), BF16),
            dma((6,)),
            dma((count, 2)),
            dma,
            dma,
            dma,
            dma((count,)),
            dma((count,)),
            dma,
            dma((count,)),
            dma,
            dma,
            dma,
            dma,
            plain,
            plain,
            plain,
        ],
        compiler_params=pltpu.CompilerParams(
            collective_id=0, has_side_effects=True, vmem_limit_bytes=60 * 1024 * 1024
        ),
    )(
        series.transpose(2, 0, 1).reshape(time_dev * probes, sens_dev),
        kernel.transpose(0, 2, 1, 3).reshape(2, depth, cols),
        prior_spectrum,
        prior_scale.reshape(1, cols),
        jnp.asarray(short),
        jnp.asarray(tabs),
        jnp.asarray(img_tab),
    )


def solution(mesh):
    placed = (P(None, "sens", "freq"), P(None, "freq", "sens", "param"), P("freq"), P("param"))
    return jax.shard_map(
        functools.partial(local, dict(mesh.shape)),
        mesh=mesh,
        in_specs=placed,
        out_specs=P("freq", "sens", "param"),
        check_vma=False,
    )
```

```python
import functools
import math

import jax
import jax.numpy as jnp
import numpy as np
from jax import lax
from jax.experimental import pallas as pl
from jax.experimental.pallas import tpu as pltpu
from jax.sharding import PartitionSpec as P

LEN = 840
MESH = pl.DeviceIdType.MESH
BF16 = jnp.bfloat16
F32 = jnp.float32
RESIDUAL = 2.0**-26
STEP = 256
LANES = 128


def split(table):
    table = table.astype(np.float32)
    high = table.astype(BF16)
    low = (table - high.astype(np.float32)).astype(BF16)
    return high, low


def phases(groups, bins_dev, time_dev):
    bins, times = groups * bins_dev, groups * time_dev
    angle = 2.0 * np.pi * ((np.arange(times)[:, None] * np.arange(bins)[None, :]) % LEN) / LEN
    both = np.stack([np.cos(angle), -np.sin(angle)], axis=1)
    both = both.reshape(times, 2, groups, bins_dev).transpose(2, 0, 1, 3)
    return both.reshape(groups, times, 2 * bins_dev)


def factor(table, multiple):
    left, size, right = np.linalg.svd(table, full_matrices=False)
    rank = size.size
    for r in range(1, size.size):
        if np.abs(table - (left[:, :r] * size[:r]) @ right[:r]).max() < RESIDUAL:
            rank = r
            break
    rank = min(-(-rank // multiple) * multiple, size.size)
    return left * size, right, rank


def with_probes(table, probes):
    full = np.einsum("...ij,qr->...iqjr", table, np.eye(probes))
    lead = table.shape[:-2]
    return full.reshape(lead + (table.shape[-2] * probes, table.shape[-1] * probes))


def series_tables(groups, bins_dev, time_dev, probes):
    comps = phases(groups, bins_dev, time_dev) / math.sqrt(groups * time_dev)
    blocks = comps.reshape(groups, groups, time_dev, 2 * bins_dev).transpose(0, 1, 3, 2)
    parts = [factor(block.reshape(-1, time_dev), 2) for block in blocks]
    rank = max(part[2] for part in parts)
    short = np.stack([right[:rank] for _, right, _ in parts])
    short = np.stack(split(with_probes(short, probes)), axis=1)
    long = np.stack([left[:, :rank] for left, _, _ in parts])
    long = long.reshape(groups, groups, 2, bins_dev, rank).transpose(0, 1, 2, 4, 3)
    long = np.stack([np.roll(long[g], -g, axis=0) for g in range(groups)])
    return short, long.reshape(groups, -1, bins_dev), rank


def image_tables(groups, bins_dev, time_dev, keep):
    comps = phases(groups, bins_dev, time_dev)
    parts = [factor(comp, 8) for comp in comps]
    rank = max(part[2] for part in parts)
    outer = np.stack([left[:, :rank] for left, _, _ in parts])
    outer = outer.reshape(groups, groups, time_dev, rank).transpose(1, 2, 0, 3)
    full = np.einsum("gthj,qr->gtqhjr", outer, np.eye(keep))
    full = full.reshape(groups, time_dev * keep, groups, rank * keep)
    own = np.stack([full[g, :, g] for g in range(groups)])
    high, low = split(full.reshape(groups, time_dev * keep, -1))
    image = np.concatenate([high, low, split(own)[0]], axis=-1)
    inner = np.stack([right[:rank] for _, right, _ in parts])
    inner = inner.reshape(groups, rank, 2, bins_dev).transpose(0, 2, 1, 3)
    return image, np.repeat(inner, keep, axis=2).reshape(groups, -1, bins_dev), rank


def body(
    cfg,
    series_hbm,
    kernel_hbm,
    prior_hbm,
    scale_hbm,
    short_hbm,
    tabs_hbm,
    img_hbm,
    out_ref,
    kbufs,
    rows,
    prior,
    scale,
    short,
    tabs,
    img_tab,
    inner,
    squeezed,
    arrived,
    spread,
    ebuf,
    left_mat,
    sbuf,
    rbuf,
    relay,
    joined,
    gath,
    lows,
    scaled,
    edges,
    halo_left,
    halo_right,
    small_sem,
    k_sem,
    g_send,
    g_recv,
    z_send,
    z_recv,
    relay_recv,
    x_send,
    x_recv,
    hl_send,
    hl_recv,
    hr_send,
    hr_recv,
    ready_x,
    ready_z,
    ready_far,
):
    groups, params, senses, chunks, direct, bins_dev, probes, squeeze = cfg
    f = lax.axis_index("freq")
    k = lax.axis_index("param")
    s = lax.axis_index("sens")
    sens_dev = rows.shape[1]
    depth = kernel_hbm.shape[1]
    padded = left_mat.shape[1] // 2
    keep = probes // senses
    each = gath.shape[2]
    cols = scale.shape[1]
    count = len(chunks)
    has_left = k > 0
    has_right = k < params - 1
    has_under = s > 0
    has_over = s < senses - 1
    outer = jnp.logical_or(s == 0, s == senses - 1)
    within = jnp.logical_not(outer)
    second = lax.rem(k, 2) == 1
    first = jnp.logical_not(second)
    pair = s + 1 - 2 * lax.rem(s, 2)
    across = senses - 1 - s
    other = senses - 1 - pair

    def freq_peer(d):
        return lax.rem(f + d, groups)

    def tell(sem, **where):
        pl.semaphore_signal(sem, inc=1, device_id=where, device_id_type=MESH)

    small = [
        pltpu.make_async_copy(series_hbm, rows, small_sem.at[0]),
        pltpu.make_async_copy(short_hbm, short, small_sem.at[1]),
        pltpu.make_async_copy(tabs_hbm.at[f], tabs, small_sem.at[2]),
        pltpu.make_async_copy(prior_hbm, prior, small_sem.at[3]),
        pltpu.make_async_copy(scale_hbm, scale, small_sem.at[4]),
        pltpu.make_async_copy(img_hbm.at[f], img_tab, small_sem.at[5]),
    ]
    for copy in small:
        copy.start()

    barrier = pltpu.get_barrier_semaphore()
    for d in range(1, groups):
        tell(barrier, freq=freq_peer(d))

    @pl.when(has_under)
    def _():
        tell(barrier, sens=s - 1)

    @pl.when(has_over)
    def _():
        tell(barrier, sens=s + 1)

    @pl.when(has_left)
    def _():
        tell(barrier, param=k - 1)

    @pl.when(has_right)
    def _():
        tell(barrier, param=k + 1)

    row = lax.broadcasted_iota(jnp.int32, spread.shape, 0)
    lane = lax.broadcasted_iota(jnp.int32, spread.shape, 1)
    spread[...] = jnp.where(lane // bins_dev == row, 1.0, 0.0).astype(BF16)
    for buf in kbufs:
        pad = jnp.zeros((padded - depth, buf.shape[1]), BF16)
        buf[depth:padded] = pad
        buf[padded + depth :] = pad

    small[0].wait()
    small[1].wait()
    loads = [
        [
            pltpu.make_async_copy(
                kernel_hbm.at[part, :, pl.ds(at, width)],
                kbufs[c].at[pl.ds(part * padded, depth)],
                k_sem.at[c, part],
            )
            for part in range(2)
        ]
        for c, (at, width) in enumerate(chunks)
    ]
    for group in loads:
        for copy in group:
            copy.start()

    series = rows[...]

    def shortened(g):
        return jnp.dot(short[g, 0], series, preferred_element_type=F32) + jnp.dot(
            short[g, 1], series, preferred_element_type=F32
        )

    for d in range(1, groups):
        g = freq_peer(d)
        squeezed[g] = shortened(g).astype(BF16)

    beside = [has_under, has_over, has_left, has_right]
    pl.semaphore_wait(barrier, groups - 1 + sum(jnp.where(b, 1, 0) for b in beside))

    def series_copy(target, slot):
        return pltpu.make_async_remote_copy(
            src_ref=squeezed.at[target],
            dst_ref=arrived.at[slot],
            send_sem=g_send,
            recv_sem=g_recv,
            device_id={"freq": target},
            device_id_type=MESH,
        )

    for d in range(1, groups):
        series_copy(freq_peer(d), f).start()
    for d in range(1, groups):
        tell(ready_x, freq=freq_peer(d))

    @pl.when(within)
    def _():
        tell(ready_z, sens=s - 1)
        tell(ready_z, sens=s + 1)

    for copy in small[2:]:
        copy.wait()
    norm = 1.0 / math.sqrt(bins_dev * groups)
    lane = lax.broadcasted_iota(jnp.int32, (8, STEP), 1) % bins_dev
    value = jnp.zeros((8, STEP), F32)
    for b in range(bins_dev):
        value = jnp.where(lane == b, prior[b] * norm, value)
    base = groups * 2 * squeeze
    for q in range(2):
        inner[q] = tabs[base + q * each : base + (q + 1) * each] * value[:1]

    cuts = [(at, min(STEP, padded - at)) for at in range(0, padded, STEP)]

    def expand(coefs, at, width):
        first = at // bins_dev // LANES * LANES
        last = min(first + LANES, sens_dev)
        return jnp.dot(
            coefs[:, first:last], spread[first:last, at : at + width], preferred_element_type=F32
        )

    def weighed(full, d, q, width):
        total = None
        for j in range(squeeze):
            at = (d * 2 + q) * squeeze + j
            term = full[j * probes : (j + 1) * probes] * tabs[at : at + 1, :width]
            total = term if total is None else total + term
        return total

    mine = shortened(f)
    high = mine.astype(BF16)
    low = (mine - high.astype(F32)).astype(BF16)
    mine = jnp.concatenate([high, low], axis=0)
    for at, width in cuts:
        full = expand(mine, at, width)
        full = full[: squeeze * probes] + full[squeeze * probes :]
        for q in range(2):
            ebuf[q, :, at : at + width] = weighed(full, 0, q, width)

    pl.semaphore_wait(ready_z, 1)

    @pl.when(within)
    def _():
        tell(ready_far, sens=pair)

    for copy in loads[0]:
        copy.wait()

    def series_done():
        return pltpu.make_async_remote_copy(
            src_ref=squeezed.at[pl.ds(0, groups - 1)],
            dst_ref=arrived.at[pl.ds(0, groups - 1)],
            send_sem=g_send,
            recv_sem=g_recv,
            device_id={"freq": freq_peer(1)},
            device_id_type=MESH,
        )

    @pl.when(within)
    def _():
        for c, (at, width) in enumerate(chunks):
            if c not in direct:
                nothing = jnp.zeros((width // LANES,) + rbuf.shape[2:], BF16)
                rbuf[other, pl.ds(at // LANES, width // LANES)] = nothing

    series_done().wait_recv()
    came = [arrived[freq_peer(d)] for d in range(1, groups)]
    head = None
    for group in [cuts[i : i + 2] for i in range(0, len(cuts), 2)]:
        for at, width in group:
            cut = slice(at, at + width)
            fulls = [expand(c, at, width) for c in came]
            for q in range(2):
                total = ebuf[q, :, cut]
                for d in range(1, groups):
                    total = total + weighed(fulls[d - 1], d, q, width)
                ebuf[q, :, cut] = total
            which = lax.broadcasted_iota(jnp.int32, (8, width), 0) % keep
            for j in range(senses):
                both = []
                for q in range(2):
                    e = jnp.broadcast_to(ebuf[q, j * keep : j * keep + 1, cut], (8, width))
                    for r in range(1, keep):
                        here = j * keep + r
                        e = jnp.where(which == r, ebuf[q, here : here + 1, cut], e)
                    both.append(jnp.concatenate([e] * (each // 8), axis=0))
                re, im = both
                one, two = inner[0, :, :width], inner[1, :, :width]
                block = slice(j * each, (j + 1) * each)
                left_mat[block, cut] = (one * re + two * im).astype(BF16)
                left_mat[block, padded + at : padded + at + width] = (one * im - two * re).astype(BF16)
        start, stop = group[0][0], group[-1][0] + group[-1][1]
        for base in (0, padded):
            term = jnp.dot(
                left_mat[:, base + start : base + stop],
                kbufs[0][base + start : base + stop],
                preferred_element_type=F32,
            )
            head = term if head is None else head + term

    def blocks(c):
        at, width = chunks[c]
        return pl.ds(at // LANES, width // LANES)

    def remote(src, dst, send, recv, **where):
        return pltpu.make_async_remote_copy(
            src_ref=src,
            dst_ref=dst,
            send_sem=send,
            recv_sem=recv,
            device_id=where,
            device_id_type=MESH,
        )

    def z_copy(target, c):
        return remote(
            sbuf.at[target, blocks(c)], rbuf.at[s, blocks(c)], z_send, z_recv.at[c], sens=target
        )

    def z_done(units, c):
        part = rbuf.at[pl.ds(0, units), blocks(c)]
        return remote(part, part, z_send, z_recv.at[c], sens=pair)

    def relay_copy(c):
        return remote(
            sbuf.at[other, blocks(c)], relay.at[blocks(c)], z_send, relay_recv.at[c], sens=pair
        )

    def joined_copy(c):
        return remote(
            joined.at[blocks(c)], rbuf.at[s, blocks(c)], z_send, z_recv.at[c], sens=across
        )

    def send_sums(c):
        if c in direct:
            for target in (across, other, pair):
                z_copy(target, c).start()
            return

        @pl.when(outer)
        def _():
            relay_copy(c).start()
            z_copy(across, c).start()
            z_copy(pair, c).start()

        @pl.when(within)
        def _():
            z_copy(other, c).start()
            z_copy(pair, c).start()

    def pass_on(c):
        if c in direct:
            return

        @pl.when(within)
        def _():
            relay_copy(c).wait_recv()
            both = sbuf[across, blocks(c)].astype(F32) + relay[blocks(c)].astype(F32)
            joined[blocks(c)] = both.astype(BF16)
            joined_copy(c).start()

    def collect(c):
        if c in direct:
            z_done(3, c).wait_recv()
        else:

            @pl.when(outer)
            def _():
                z_done(3, c).wait_recv()

            @pl.when(within)
            def _():
                z_done(2, c).wait_recv()

        total = sbuf[s, blocks(c)].astype(F32)
        for slot in (pair, other, across):
            total = total + rbuf[slot, blocks(c)].astype(F32)
        return total

    for c, (at, width) in enumerate(chunks):
        if c > 0:
            for copy in loads[c]:
                copy.wait()
        total = head
        if c > 0:
            total = jnp.dot(left_mat[...], kbufs[c][...], preferred_element_type=F32)
        total = total.astype(BF16)
        for j in range(senses):
            for b in range(width // LANES):
                sbuf[j, at // LANES + b] = total[
                    j * each : (j + 1) * each, b * LANES : (b + 1) * LANES
                ]
        if c == 0:

            @pl.when(outer)
            def _():
                pl.semaphore_wait(ready_far, 1)

        send_sums(c)

    def x_copy(target, c):
        part = gath.at[f, blocks(c)]
        return remote(part, part, x_send, x_recv.at[c], freq=target)

    def x_done(c):
        part = gath.at[pl.ds(0, groups - 1), blocks(c)]
        return remote(part, part, x_send, x_recv.at[c], freq=freq_peer(1))

    def to_left(target):
        return remote(
            edges.at[0],
            halo_right.at[f],
            hl_send,
            hr_recv,
            freq=target,
            param=jnp.maximum(k - 1, 0),
        )

    def to_right(target):
        return remote(
            edges.at[1],
            halo_left.at[f],
            hr_send,
            hl_recv,
            freq=target,
            param=jnp.minimum(k + 1, params - 1),
        )

    def image_of(stack, low):
        wide = 2 * groups * each
        full = jnp.concatenate(stack + stack + ([] if low is None else [low]), axis=0)
        table = img_tab[:, : wide if low is None else wide + each]
        return jnp.dot(table, full, preferred_element_type=F32)

    def across_lanes(parts):
        return parts[0] if len(parts) == 1 else jnp.concatenate(parts, axis=1)

    def finish(c):
        x_done(c).wait_recv()
        at, width = chunks[c]
        span = range(at // LANES, (at + width) // LANES)
        stack = [across_lanes([gath[g, b] for b in span]) for g in range(groups)]
        image = image_of(stack, across_lanes([lows[b] for b in span]))
        scaled[:, at : at + width] = image * scale[:, at : at + width]

    pl.semaphore_wait(ready_x, groups - 1)
    for c in range(count):
        pass_on(c)
    for c, (at, width) in enumerate(chunks):
        total = collect(c)
        high = total.astype(BF16)
        gath[f, blocks(c)] = high
        for d in range(1, groups):
            x_copy(freq_peer(d), c).start()
        lows[blocks(c)] = (total - high.astype(F32)).astype(BF16)
        if at == 0:
            edges[0] = (total[0] * scale[:, :LANES]).astype(BF16)

            @pl.when(has_left)
            def _():
                for d in range(groups):
                    to_left(freq_peer(d)).start()

        if at + width == cols:
            edges[1] = (total[width // LANES - 1] * scale[:, cols - LANES :]).astype(BF16)

            @pl.when(has_right)
            def _():
                for d in range(groups):
                    to_right(freq_peer(d)).start()

    for c in range(count - 1):
        finish(c)

    def halo_done(ref, send, recv):
        return remote(ref, ref, send, recv, freq=freq_peer(1))

    @pl.when(has_left)
    def _():
        halo_done(halo_left, hr_send, hl_recv).wait_recv()

    @pl.when(jnp.logical_not(has_left))
    def _():
        halo_left[...] = jnp.zeros_like(halo_left)

    @pl.when(has_right)
    def _():
        halo_done(halo_right, hl_send, hr_recv).wait_recv()

    @pl.when(jnp.logical_not(has_right))
    def _():
        halo_right[...] = jnp.zeros_like(halo_right)

    left = image_of([halo_left[g] for g in range(groups)], None)
    right = image_of([halo_right[g] for g in range(groups)], None)
    def smooth(at, end):
        if at >= end:
            return
        mid = scaled[:, at:end]
        before = scaled[:, at - 1 : at] if at > 0 else left[:, LANES - 1 :]
        after = scaled[:, end : end + 1] if end < cols else right[:, :1]
        lower = jnp.concatenate([before, mid[:, :-1]], axis=1)
        upper = jnp.concatenate([mid[:, 1:], after], axis=1)
        value = scale[:, at:end] * (0.5 * mid + 0.25 * (lower + upper))
        out_ref[:, :, at:end] = value.reshape(out_ref.shape[0], keep, end - at)

    at, width = chunks[-1]
    start, stop = max(at - LANES, 0), min(at + width + LANES, cols)
    smooth(0, start)
    smooth(stop, cols)
    finish(count - 1)
    smooth(start, stop)

    series_done().wait_send()
    part = sbuf.at[pl.ds(0, 3)]
    remote(part, part, z_send, z_recv.at[0], sens=pair).wait_send()
    part = gath.at[pl.ds(0, groups - 1)]
    remote(part, part, x_send, x_recv.at[0], freq=freq_peer(1)).wait_send()

    @pl.when(has_left)
    def _():
        halo_done(halo_right, hl_send, hr_recv).wait_send()

    @pl.when(has_right)
    def _():
        halo_done(halo_left, hr_send, hl_recv).wait_send()


def local(mesh_shape, series, kernel, prior_spectrum, prior_scale):
    groups, params, senses = (mesh_shape[n] for n in ("freq", "param", "sens"))
    assert senses == 4 and groups > 1
    probes, sens_dev, time_dev = series.shape
    _, bins_dev, _, cols = kernel.shape
    keep = probes // senses
    quarter = cols // 4
    chunks = [(0, quarter), (3 * quarter, quarter), (quarter, quarter), (2 * quarter, quarter)]
    direct = (len(chunks) - 1,)
    count = len(chunks)
    depth = sens_dev * bins_dev
    padded = -(-depth // LANES) * LANES
    short, long, squeeze = series_tables(groups, bins_dev, time_dev, probes)
    img_tab, inner, rank = image_tables(groups, bins_dev, time_dev, keep)
    tabs = np.concatenate([long, inner], axis=1)
    tabs = np.tile(tabs, (1, 1, STEP // bins_dev)).astype(np.float32)
    each = rank * keep
    spans = cols // LANES
    dma = pltpu.SemaphoreType.DMA
    plain = pltpu.SemaphoreType.REGULAR
    return pl.pallas_call(
        functools.partial(
            body, (groups, params, senses, chunks, direct, bins_dev, probes, squeeze)
        ),
        out_shape=pltpu.VMEM((time_dev, keep, cols), F32),
        in_specs=[pl.BlockSpec(memory_space=pltpu.HBM)] * 7,
        out_specs=pl.BlockSpec(memory_space=pltpu.VMEM),
        scratch_shapes=[
            [pltpu.VMEM((2 * padded, width), BF16) for _, width in chunks],
            pltpu.VMEM((time_dev * probes, sens_dev), BF16),
            pltpu.SMEM((bins_dev,), F32),
            pltpu.VMEM((1, cols), F32),
            pltpu.VMEM(short.shape, BF16),
            pltpu.VMEM(tabs.shape[1:], F32),
            pltpu.VMEM(img_tab.shape[1:], BF16),
            pltpu.VMEM((2, each, STEP), F32),
            pltpu.VMEM((groups, squeeze * probes, sens_dev), BF16),
            pltpu.VMEM((groups, squeeze * probes, sens_dev), BF16),
            pltpu.VMEM((sens_dev, padded), BF16),
            pltpu.VMEM((2, probes, padded), F32),
            pltpu.VMEM((senses * each, 2 * padded), BF16),
            pltpu.VMEM((senses, spans, each, LANES), BF16),
            pltpu.VMEM((senses, spans, each, LANES), BF16),
            pltpu.VMEM((spans, each, LANES), BF16),
            pltpu.VMEM((spans, each, LANES), BF16),
            pltpu.VMEM((groups, spans, each, LANES), BF16),
            pltpu.VMEM((spans, each, LANES), BF16),
            pltpu.VMEM((time_dev * keep, cols), F32),
            pltpu.VMEM((2, each, LANES), BF16),
            pltpu.VMEM((groups, each, LANES), BF16),
            pltpu.VMEM((groups, each, LANES), BF16),
            dma((6,)),
            dma((count, 2)),
            dma,
            dma,
            dma,
            dma((count,)),
            dma((count,)),
            dma,
            dma((count,)),
            dma,
            dma,
            dma,
            dma,
            plain,
            plain,
            plain,
        ],
        compiler_params=pltpu.CompilerParams(
            collective_id=0, has_side_effects=True, vmem_limit_bytes=60 * 1024 * 1024
        ),
    )(
        series.transpose(2, 0, 1).reshape(time_dev * probes, sens_dev),
        kernel.transpose(0, 2, 1, 3).reshape(2, depth, cols),
        prior_spectrum,
        prior_scale.reshape(1, cols),
        jnp.asarray(short),
        jnp.asarray(tabs),
        jnp.asarray(img_tab),
    )


def solution(mesh):
    placed = (P(None, "sens", "freq"), P(None, "freq", "sens", "param"), P("freq"), P("param"))
    return jax.shard_map(
        functools.partial(local, dict(mesh.shape)),
        mesh=mesh,
        in_specs=placed,
        out_specs=P("freq", "sens", "param"),
        check_vma=False,
    )
```

```python
import functools
import math

import jax
import jax.numpy as jnp
import numpy as np
from jax import lax
from jax.experimental import pallas as pl
from jax.experimental.pallas import tpu as pltpu
from jax.sharding import PartitionSpec as P

LEN = 840
MESH = pl.DeviceIdType.MESH
BF16 = jnp.bfloat16
F32 = jnp.float32
RESIDUAL = 2.0**-26
STEP = 256
LANES = 128


def split(table):
    table = table.astype(np.float32)
    high = table.astype(BF16)
    low = (table - high.astype(np.float32)).astype(BF16)
    return high, low


def phases(groups, bins_dev, time_dev):
    bins, times = groups * bins_dev, groups * time_dev
    angle = 2.0 * np.pi * ((np.arange(times)[:, None] * np.arange(bins)[None, :]) % LEN) / LEN
    both = np.stack([np.cos(angle), -np.sin(angle)], axis=1)
    both = both.reshape(times, 2, groups, bins_dev).transpose(2, 0, 1, 3)
    return both.reshape(groups, times, 2 * bins_dev)


def factor(table, multiple):
    left, size, right = np.linalg.svd(table, full_matrices=False)
    rank = size.size
    for r in range(1, size.size):
        if np.abs(table - (left[:, :r] * size[:r]) @ right[:r]).max() < RESIDUAL:
            rank = r
            break
    rank = min(-(-rank // multiple) * multiple, size.size)
    return left * size, right, rank


def with_probes(table, probes):
    full = np.einsum("...ij,qr->...iqjr", table, np.eye(probes))
    lead = table.shape[:-2]
    return full.reshape(lead + (table.shape[-2] * probes, table.shape[-1] * probes))


def series_tables(groups, bins_dev, time_dev, probes):
    comps = phases(groups, bins_dev, time_dev) / math.sqrt(groups * time_dev)
    blocks = comps.reshape(groups, groups, time_dev, 2 * bins_dev).transpose(0, 1, 3, 2)
    parts = [factor(block.reshape(-1, time_dev), 2) for block in blocks]
    rank = max(part[2] for part in parts)
    short = np.stack([right[:rank] for _, right, _ in parts])
    short = np.stack(split(with_probes(short, probes)), axis=1)
    long = np.stack([left[:, :rank] for left, _, _ in parts])
    long = long.reshape(groups, groups, 2, bins_dev, rank).transpose(0, 1, 2, 4, 3)
    long = np.stack([np.roll(long[g], -g, axis=0) for g in range(groups)])
    return short, long.reshape(groups, -1, bins_dev), rank


def packing(each):
    whole = each // 8 * 8
    first = np.concatenate([np.arange(whole), 2 * whole + np.arange(each - whole)])
    second = np.concatenate([whole + np.arange(whole), whole + each + np.arange(each - whole)])
    return first, second


def image_tables(groups, bins_dev, time_dev, keep):
    comps = phases(groups, bins_dev, time_dev)
    parts = [factor(comp, 2) for comp in comps]
    rank = max(part[2] for part in parts)
    each, rows = rank * keep, time_dev * keep
    outer = np.stack([left[:, :rank] for left, _, _ in parts])
    outer = outer.reshape(groups, groups, time_dev, rank).transpose(1, 0, 2, 3)
    full = np.einsum("ghtj,qr->ghtqjr", outer, np.eye(keep))
    full = full.reshape(groups, groups, rows, each)
    tall = -(-rows // 8) * 8
    packed = np.zeros((groups, groups, 2 * tall, 2 * each))
    for half, places in enumerate(packing(each)):
        packed[:, :, half * tall : half * tall + rows, places] = full
    high, low = split(packed)
    own = np.stack([high[g, g] for g in range(groups)])
    image = np.concatenate([high, low, own[:, None]], axis=1)
    inner = np.stack([right[:rank] for _, right, _ in parts])
    inner = inner.reshape(groups, rank, 2, bins_dev).transpose(0, 2, 1, 3)
    inner = np.repeat(inner, keep, axis=2)
    slot = -(-each // 8) * 8
    inner = np.pad(inner, ((0, 0), (0, 0), (0, slot - each), (0, 0)))
    return image, inner.reshape(groups, -1, bins_dev), each, slot


def body(
    cfg,
    series_hbm,
    kernel_hbm,
    prior_hbm,
    scale_hbm,
    short_hbm,
    tabs_hbm,
    img_hbm,
    out_ref,
    kbufs,
    rows,
    prior,
    scale,
    short,
    tabs,
    img_tab,
    inner,
    squeezed,
    arrived,
    spread,
    ebuf,
    left_mat,
    sbuf,
    rbuf,
    relay,
    joined,
    gath,
    lows,
    scaled,
    edges,
    halo_left,
    halo_right,
    small_sem,
    k_sem,
    g_send,
    g_recv,
    z_send,
    z_recv,
    relay_recv,
    x_send,
    x_recv,
    hl_send,
    hl_recv,
    hr_send,
    hr_recv,
    ready_x,
    ready_z,
    ready_far,
):
    groups, params, senses, chunks, direct, bins_dev, probes, squeeze, each = cfg
    f = lax.axis_index("freq")
    k = lax.axis_index("param")
    s = lax.axis_index("sens")
    sens_dev = rows.shape[1]
    depth = kernel_hbm.shape[1]
    padded = left_mat.shape[1] // 2
    keep = probes // senses
    slot = inner.shape[1]
    width = 2 * LANES
    cols = scale.shape[1]
    count = len(chunks)
    has_left = k > 0
    has_right = k < params - 1
    has_under = s > 0
    has_over = s < senses - 1
    outer = jnp.logical_or(s == 0, s == senses - 1)
    within = jnp.logical_not(outer)
    second = lax.rem(k, 2) == 1
    first = jnp.logical_not(second)
    pair = s + 1 - 2 * lax.rem(s, 2)
    across = senses - 1 - s
    other = senses - 1 - pair

    def freq_peer(d):
        return lax.rem(f + d, groups)

    def tell(sem, **where):
        pl.semaphore_signal(sem, inc=1, device_id=where, device_id_type=MESH)

    small = [
        pltpu.make_async_copy(series_hbm, rows, small_sem.at[0]),
        pltpu.make_async_copy(short_hbm, short, small_sem.at[1]),
        pltpu.make_async_copy(tabs_hbm.at[f], tabs, small_sem.at[2]),
        pltpu.make_async_copy(prior_hbm, prior, small_sem.at[3]),
        pltpu.make_async_copy(scale_hbm, scale, small_sem.at[4]),
        pltpu.make_async_copy(img_hbm.at[f], img_tab, small_sem.at[5]),
    ]
    for copy in small:
        copy.start()

    barrier = pltpu.get_barrier_semaphore()
    for d in range(1, groups):
        tell(barrier, freq=freq_peer(d))

    @pl.when(has_under)
    def _():
        tell(barrier, sens=s - 1)

    @pl.when(has_over)
    def _():
        tell(barrier, sens=s + 1)

    @pl.when(has_left)
    def _():
        tell(barrier, param=k - 1)

    @pl.when(has_right)
    def _():
        tell(barrier, param=k + 1)

    row = lax.broadcasted_iota(jnp.int32, spread.shape, 0)
    lane = lax.broadcasted_iota(jnp.int32, spread.shape, 1)
    spread[...] = jnp.where(lane // bins_dev == row, 1.0, 0.0).astype(BF16)
    for buf in kbufs:
        pad = jnp.zeros((padded - depth, buf.shape[1]), BF16)
        buf[depth:padded] = pad
        buf[padded + depth :] = pad

    small[0].wait()
    small[1].wait()
    loads = [
        [
            pltpu.make_async_copy(
                kernel_hbm.at[part, :, pl.ds(at, width)],
                kbufs[c].at[pl.ds(part * padded, depth)],
                k_sem.at[c, part],
            )
            for part in range(2)
        ]
        for c, at in enumerate(chunks)
    ]
    for group in loads:
        for copy in group:
            copy.start()

    series = rows[...]

    def shortened(g):
        return jnp.dot(short[g, 0], series, preferred_element_type=F32) + jnp.dot(
            short[g, 1], series, preferred_element_type=F32
        )

    for d in range(1, groups):
        g = freq_peer(d)
        squeezed[g] = shortened(g).astype(BF16)

    beside = [has_under, has_over, has_left, has_right]
    pl.semaphore_wait(barrier, groups - 1 + sum(jnp.where(b, 1, 0) for b in beside))

    def series_copy(target, slot):
        return pltpu.make_async_remote_copy(
            src_ref=squeezed.at[target],
            dst_ref=arrived.at[slot],
            send_sem=g_send,
            recv_sem=g_recv,
            device_id={"freq": target},
            device_id_type=MESH,
        )

    for d in range(1, groups):
        series_copy(freq_peer(d), f).start()
    for d in range(1, groups):
        tell(ready_x, freq=freq_peer(d))

    @pl.when(within)
    def _():
        tell(ready_z, sens=s - 1)
        tell(ready_z, sens=s + 1)

    for copy in small[2:]:
        copy.wait()
    norm = 1.0 / math.sqrt(bins_dev * groups)
    lane = lax.broadcasted_iota(jnp.int32, (8, STEP), 1) % bins_dev
    value = jnp.zeros((8, STEP), F32)
    for b in range(bins_dev):
        value = jnp.where(lane == b, prior[b] * norm, value)
    base = groups * 2 * squeeze
    for q in range(2):
        inner[q] = tabs[base + q * slot : base + (q + 1) * slot] * value[:1]

    cuts = [(at, min(STEP, padded - at)) for at in range(0, padded, STEP)]

    def expand(coefs, at, span):
        first = at // bins_dev // LANES * LANES
        last = min(first + LANES, sens_dev)
        return jnp.dot(
            coefs[:, first:last], spread[first:last, at : at + span], preferred_element_type=F32
        )

    def weighed(full, d, q, span):
        total = None
        for j in range(squeeze):
            at = (d * 2 + q) * squeeze + j
            term = full[j * probes : (j + 1) * probes] * tabs[at : at + 1, :span]
            total = term if total is None else total + term
        return total

    mine = shortened(f)
    high = mine.astype(BF16)
    low = (mine - high.astype(F32)).astype(BF16)
    mine = jnp.concatenate([high, low], axis=0)
    for at, span in cuts:
        full = expand(mine, at, span)
        full = full[: squeeze * probes] + full[squeeze * probes :]
        for q in range(2):
            ebuf[q, :, at : at + span] = weighed(full, 0, q, span)

    pl.semaphore_wait(ready_z, 1)

    @pl.when(within)
    def _():
        tell(ready_far, sens=pair)

    for copy in loads[0]:
        copy.wait()

    def series_done():
        return pltpu.make_async_remote_copy(
            src_ref=squeezed.at[pl.ds(0, groups - 1)],
            dst_ref=arrived.at[pl.ds(0, groups - 1)],
            send_sem=g_send,
            recv_sem=g_recv,
            device_id={"freq": freq_peer(1)},
            device_id_type=MESH,
        )

    @pl.when(within)
    def _():
        for c in range(count):
            if c not in direct:
                rbuf[other, c] = jnp.zeros(rbuf.shape[2:], BF16)

    series_done().wait_recv()
    came = [arrived[freq_peer(d)] for d in range(1, groups)]
    head = None
    for group in [cuts[i : i + 2] for i in range(0, len(cuts), 2)]:
        for at, span in group:
            cut = slice(at, at + span)
            fulls = [expand(c, at, span) for c in came]
            for q in range(2):
                total = ebuf[q, :, cut]
                for d in range(1, groups):
                    total = total + weighed(fulls[d - 1], d, q, span)
                ebuf[q, :, cut] = total
            which = lax.broadcasted_iota(jnp.int32, (8, span), 0) % keep
            for j in range(senses):
                both = []
                for q in range(2):
                    e = jnp.broadcast_to(ebuf[q, j * keep : j * keep + 1, cut], (8, span))
                    for r in range(1, keep):
                        here = j * keep + r
                        e = jnp.where(which == r, ebuf[q, here : here + 1, cut], e)
                    both.append(jnp.concatenate([e] * (slot // 8), axis=0))
                re, im = both
                one, two = inner[0, :, :span], inner[1, :, :span]
                block = slice(j * slot, (j + 1) * slot)
                left_mat[block, cut] = (one * re + two * im).astype(BF16)
                left_mat[block, padded + at : padded + at + span] = (one * im - two * re).astype(BF16)
        start, stop = group[0][0], group[-1][0] + group[-1][1]
        for base in (0, padded):
            term = jnp.dot(
                left_mat[:, base + start : base + stop],
                kbufs[0][base + start : base + stop],
                preferred_element_type=F32,
            )
            head = term if head is None else head + term

    def remote(src, dst, send, recv, **where):
        return pltpu.make_async_remote_copy(
            src_ref=src,
            dst_ref=dst,
            send_sem=send,
            recv_sem=recv,
            device_id=where,
            device_id_type=MESH,
        )

    def z_copy(target, c):
        return remote(
            sbuf.at[target, c], rbuf.at[s, c], z_send, z_recv.at[c], sens=target
        )

    def z_done(units, c):
        part = rbuf.at[pl.ds(0, units), c]
        return remote(part, part, z_send, z_recv.at[c], sens=pair)

    def relay_copy(c):
        return remote(
            sbuf.at[other, c], relay.at[c], z_send, relay_recv.at[c], sens=pair
        )

    def joined_copy(c):
        return remote(
            joined.at[c], rbuf.at[s, c], z_send, z_recv.at[c], sens=across
        )

    def send_sums(c):
        if c in direct:
            for target in (across, other, pair):
                z_copy(target, c).start()
            return

        @pl.when(outer)
        def _():
            relay_copy(c).start()
            z_copy(across, c).start()
            z_copy(pair, c).start()

        @pl.when(within)
        def _():
            z_copy(other, c).start()
            z_copy(pair, c).start()

    def pass_on(c):
        if c in direct:
            return

        @pl.when(within)
        def _():
            relay_copy(c).wait_recv()
            both = sbuf[across, c].astype(F32) + relay[c].astype(F32)
            joined[c] = both.astype(BF16)
            joined_copy(c).start()

    def collect(c):
        if c in direct:
            z_done(3, c).wait_recv()
        else:

            @pl.when(outer)
            def _():
                z_done(3, c).wait_recv()

            @pl.when(within)
            def _():
                z_done(2, c).wait_recv()

        total = sbuf[s, c].astype(F32)
        for slot in (pair, other, across):
            total = total + rbuf[slot, c].astype(F32)
        return total

    whole = each // 8 * 8
    for c in range(count):
        if c > 0:
            for copy in loads[c]:
                copy.wait()
        total = head
        if c > 0:
            total = jnp.dot(left_mat[...], kbufs[c][...], preferred_element_type=F32)
        for j in range(senses):
            halves = [
                total[j * slot : (j + 1) * slot, h * LANES : (h + 1) * LANES] for h in range(2)
            ]
            packed = [half[:whole] for half in halves]
            if slot > each:
                packed.append(halves[0][whole:] + pltpu.roll(halves[1][whole:], each - whole, 0))
            sbuf[j, c] = jnp.concatenate(packed, axis=0).astype(BF16)
        if c == 0:

            @pl.when(outer)
            def _():
                pl.semaphore_wait(ready_far, 1)

        send_sums(c)

    def x_copy(target, c):
        part = gath.at[f, c]
        return remote(part, part, x_send, x_recv.at[c], freq=target)

    def x_done(c):
        part = gath.at[pl.ds(0, groups - 1), c]
        return remote(part, part, x_send, x_recv.at[c], freq=freq_peer(1))

    def to_left(target):
        return remote(
            edges.at[0],
            halo_right.at[f],
            hl_send,
            hr_recv,
            freq=target,
            param=jnp.maximum(k - 1, 0),
        )

    def to_right(target):
        return remote(
            edges.at[1],
            halo_left.at[f],
            hr_send,
            hl_recv,
            freq=target,
            param=jnp.minimum(k + 1, params - 1),
        )

    rows_out = scaled.shape[0]
    tall = img_tab.shape[1] // 2

    def image_of(pieces):
        total = None
        for index, piece in pieces:
            term = jnp.dot(img_tab[index], piece, preferred_element_type=F32)
            total = term if total is None else total + term
        return total[:rows_out], total[tall : tall + rows_out]

    def twice(pieces):
        return list(enumerate(pieces + pieces))

    def finish(c):
        x_done(c).wait_recv()
        pieces = twice([gath[g, c] for g in range(groups)]) + [(2 * groups, lows[c])]
        for half, image in enumerate(image_of(pieces)):
            at = chunks[c] + half * LANES
            scaled[:, at : at + LANES] = image * scale[:, at : at + LANES]

    pl.semaphore_wait(ready_x, groups - 1)
    for c in range(count):
        pass_on(c)
    for c, at in enumerate(chunks):
        total = collect(c)
        high = total.astype(BF16)
        gath[f, c] = high
        for d in range(1, groups):
            x_copy(freq_peer(d), c).start()
        lows[c] = (total - high.astype(F32)).astype(BF16)
        if at == 0:
            edges[0] = (total * scale[:, :LANES]).astype(BF16)

            @pl.when(has_left)
            def _():
                for d in range(groups):
                    to_left(freq_peer(d)).start()

        if at + width == cols:
            edges[1] = (total * scale[:, cols - LANES :]).astype(BF16)

            @pl.when(has_right)
            def _():
                for d in range(groups):
                    to_right(freq_peer(d)).start()

    for c in range(count - 1):
        finish(c)

    def halo_done(ref, send, recv):
        return remote(ref, ref, send, recv, freq=freq_peer(1))

    @pl.when(has_left)
    def _():
        halo_done(halo_left, hr_send, hl_recv).wait_recv()

    @pl.when(jnp.logical_not(has_left))
    def _():
        halo_left[...] = jnp.zeros_like(halo_left)

    @pl.when(has_right)
    def _():
        halo_done(halo_right, hl_send, hr_recv).wait_recv()

    @pl.when(jnp.logical_not(has_right))
    def _():
        halo_right[...] = jnp.zeros_like(halo_right)

    _, left = image_of(twice([halo_left[g] for g in range(groups)]))
    right, _ = image_of(twice([halo_right[g] for g in range(groups)]))
    def smooth(at, end):
        if at >= end:
            return
        mid = scaled[:, at:end]
        before = scaled[:, at - 1 : at] if at > 0 else left[:, LANES - 1 :]
        after = scaled[:, end : end + 1] if end < cols else right[:, :1]
        lower = jnp.concatenate([before, mid[:, :-1]], axis=1)
        upper = jnp.concatenate([mid[:, 1:], after], axis=1)
        value = scale[:, at:end] * (0.5 * mid + 0.25 * (lower + upper))
        out_ref[:, :, at:end] = value.reshape(out_ref.shape[0], keep, end - at)

    at = chunks[-1]
    start, stop = max(at - LANES, 0), min(at + width + LANES, cols)
    smooth(0, start)
    smooth(stop, cols)
    finish(count - 1)
    smooth(start, stop)

    series_done().wait_send()
    part = sbuf.at[pl.ds(0, 3)]
    remote(part, part, z_send, z_recv.at[0], sens=pair).wait_send()
    part = gath.at[pl.ds(0, groups - 1)]
    remote(part, part, x_send, x_recv.at[0], freq=freq_peer(1)).wait_send()

    @pl.when(has_left)
    def _():
        halo_done(halo_right, hl_send, hr_recv).wait_send()

    @pl.when(has_right)
    def _():
        halo_done(halo_left, hr_send, hl_recv).wait_send()


def local(mesh_shape, series, kernel, prior_spectrum, prior_scale):
    groups, params, senses = (mesh_shape[n] for n in ("freq", "param", "sens"))
    assert senses == 4 and groups > 1
    probes, sens_dev, time_dev = series.shape
    _, bins_dev, _, cols = kernel.shape
    keep = probes // senses
    width = 2 * LANES
    assert cols % width == 0
    chunks = list(range(0, cols, width))
    chunks = chunks[:1] + chunks[:0:-1][:1] + chunks[1:-1]
    direct = (len(chunks) - 1,)
    count = len(chunks)
    depth = sens_dev * bins_dev
    padded = -(-depth // LANES) * LANES
    short, long, squeeze = series_tables(groups, bins_dev, time_dev, probes)
    img_tab, inner, each, slot = image_tables(groups, bins_dev, time_dev, keep)
    tabs = np.concatenate([long, inner], axis=1)
    tabs = np.tile(tabs, (1, 1, STEP // bins_dev)).astype(np.float32)
    unit = (2 * each, LANES)
    dma = pltpu.SemaphoreType.DMA
    plain = pltpu.SemaphoreType.REGULAR
    return pl.pallas_call(
        functools.partial(
            body, (groups, params, senses, chunks, direct, bins_dev, probes, squeeze, each)
        ),
        out_shape=pltpu.VMEM((time_dev, keep, cols), F32),
        in_specs=[pl.BlockSpec(memory_space=pltpu.HBM)] * 7,
        out_specs=pl.BlockSpec(memory_space=pltpu.VMEM),
        scratch_shapes=[
            [pltpu.VMEM((2 * padded, width), BF16) for _ in chunks],
            pltpu.VMEM((time_dev * probes, sens_dev), BF16),
            pltpu.SMEM((bins_dev,), F32),
            pltpu.VMEM((1, cols), F32),
            pltpu.VMEM(short.shape, BF16),
            pltpu.VMEM(tabs.shape[1:], F32),
            pltpu.VMEM(img_tab.shape[1:], BF16),
            pltpu.VMEM((2, slot, STEP), F32),
            pltpu.VMEM((groups, squeeze * probes, sens_dev), BF16),
            pltpu.VMEM((groups, squeeze * probes, sens_dev), BF16),
            pltpu.VMEM((sens_dev, padded), BF16),
            pltpu.VMEM((2, probes, padded), F32),
            pltpu.VMEM((senses * slot, 2 * padded), BF16),
            pltpu.VMEM((senses, count) + unit, BF16),
            pltpu.VMEM((senses, count) + unit, BF16),
            pltpu.VMEM((count,) + unit, BF16),
            pltpu.VMEM((count,) + unit, BF16),
            pltpu.VMEM((groups, count) + unit, BF16),
            pltpu.VMEM((count,) + unit, BF16),
            pltpu.VMEM((time_dev * keep, cols), F32),
            pltpu.VMEM((2,) + unit, BF16),
            pltpu.VMEM((groups,) + unit, BF16),
            pltpu.VMEM((groups,) + unit, BF16),
            dma((6,)),
            dma((count, 2)),
            dma,
            dma,
            dma,
            dma((count,)),
            dma((count,)),
            dma,
            dma((count,)),
            dma,
            dma,
            dma,
            dma,
            plain,
            plain,
            plain,
        ],
        compiler_params=pltpu.CompilerParams(
            collective_id=0, has_side_effects=True, vmem_limit_bytes=60 * 1024 * 1024
        ),
    )(
        series.transpose(2, 0, 1).reshape(time_dev * probes, sens_dev),
        kernel.transpose(0, 2, 1, 3).reshape(2, depth, cols),
        prior_spectrum,
        prior_scale.reshape(1, cols),
        jnp.asarray(short),
        jnp.asarray(tabs),
        jnp.asarray(img_tab),
    )


def solution(mesh):
    placed = (P(None, "sens", "freq"), P(None, "freq", "sens", "param"), P("freq"), P("param"))
    return jax.shard_map(
        functools.partial(local, dict(mesh.shape)),
        mesh=mesh,
        in_specs=placed,
        out_specs=P("freq", "sens", "param"),
        check_vma=False,
    )
```

```python
import functools
import math

import jax
import jax.numpy as jnp
import numpy as np
from jax import lax
from jax.experimental import pallas as pl
from jax.experimental.pallas import tpu as pltpu
from jax.sharding import PartitionSpec as P

LEN = 840
MESH = pl.DeviceIdType.MESH
BF16 = jnp.bfloat16
F32 = jnp.float32
RESIDUAL = 2.0**-26
STEP = 256
LANES = 128
PAIR = 16


def split(table):
    table = table.astype(np.float32)
    high = table.astype(BF16)
    low = (table - high.astype(np.float32)).astype(BF16)
    return high, low


def phases(groups, bins_dev, time_dev):
    bins, times = groups * bins_dev, groups * time_dev
    angle = 2.0 * np.pi * ((np.arange(times)[:, None] * np.arange(bins)[None, :]) % LEN) / LEN
    both = np.stack([np.cos(angle), -np.sin(angle)], axis=1)
    both = both.reshape(times, 2, groups, bins_dev).transpose(2, 0, 1, 3)
    return both.reshape(groups, times, 2 * bins_dev)


def factor(table, multiple):
    left, size, right = np.linalg.svd(table, full_matrices=False)
    rank = size.size
    for r in range(1, size.size):
        if np.abs(table - (left[:, :r] * size[:r]) @ right[:r]).max() < RESIDUAL:
            rank = r
            break
    rank = min(-(-rank // multiple) * multiple, size.size)
    return left * size, right, rank


def with_probes(table, probes):
    full = np.einsum("...ij,qr->...iqjr", table, np.eye(probes))
    lead = table.shape[:-2]
    return full.reshape(lead + (table.shape[-2] * probes, table.shape[-1] * probes))


def series_tables(groups, bins_dev, time_dev, probes):
    comps = phases(groups, bins_dev, time_dev) / math.sqrt(groups * time_dev)
    blocks = comps.reshape(groups, groups, time_dev, 2 * bins_dev).transpose(0, 1, 3, 2)
    parts = [factor(block.reshape(-1, time_dev), 2) for block in blocks]
    rank = max(part[2] for part in parts)
    short = np.stack([right[:rank] for _, right, _ in parts])
    short = np.stack(split(with_probes(short, probes)), axis=1)
    long = np.stack([left[:, :rank] for left, _, _ in parts])
    long = long.reshape(groups, groups, 2, bins_dev, rank).transpose(0, 1, 2, 4, 3)
    long = np.stack([np.roll(long[g], -g, axis=0) for g in range(groups)])
    return short, long.reshape(groups, -1, bins_dev), rank


def packing(each):
    whole = each // 8 * 8
    first = np.concatenate([np.arange(whole), 2 * whole + np.arange(each - whole)])
    second = np.concatenate([whole + np.arange(whole), whole + each + np.arange(each - whole)])
    return first, second


def image_tables(groups, bins_dev, time_dev, keep):
    comps = phases(groups, bins_dev, time_dev)
    parts = [factor(comp, 2) for comp in comps]
    rank = max(part[2] for part in parts)
    each, rows = rank * keep, time_dev * keep
    outer = np.stack([left[:, :rank] for left, _, _ in parts])
    outer = outer.reshape(groups, groups, time_dev, rank).transpose(1, 0, 2, 3)
    full = np.einsum("ghtj,qr->ghtqjr", outer, np.eye(keep))
    full = full.reshape(groups, groups, rows, each)
    tall = -(-rows // 8) * 8
    packed = np.zeros((groups, groups, 2 * tall, 2 * each))
    for half, places in enumerate(packing(each)):
        packed[:, :, half * tall : half * tall + rows, places] = full
    high, low = split(packed)
    own = np.stack([high[g, g] for g in range(groups)])
    image = np.concatenate([high, low, own[:, None]], axis=1)
    inner = np.stack([right[:rank] for _, right, _ in parts])
    inner = inner.reshape(groups, rank, 2, bins_dev).transpose(0, 2, 1, 3)
    inner = np.repeat(inner, keep, axis=2)
    slot = -(-each // 8) * 8
    inner = np.pad(inner, ((0, 0), (0, 0), (0, slot - each), (0, 0)))
    return image, inner.reshape(groups, -1, bins_dev), each, slot


def body(
    cfg,
    series_hbm,
    kernel_hbm,
    prior_hbm,
    scale_hbm,
    short_hbm,
    tabs_hbm,
    img_hbm,
    out_ref,
    kbufs,
    rows,
    prior,
    scale,
    short,
    tabs,
    img_tab,
    inner,
    squeezed,
    arrived,
    spread,
    ebuf,
    left_mat,
    sbuf,
    rbuf,
    relay,
    joined,
    gath,
    lows,
    scaled,
    edges,
    halo_left,
    halo_right,
    small_sem,
    k_sem,
    g_send,
    g_recv,
    z_send,
    z_recv,
    relay_recv,
    x_send,
    x_recv,
    hl_send,
    hl_recv,
    hr_send,
    hr_recv,
    ready_x,
    ready_z,
    ready_far,
):
    groups, params, senses, chunks, direct, bins_dev, probes, squeeze, each = cfg
    f = lax.axis_index("freq")
    k = lax.axis_index("param")
    s = lax.axis_index("sens")
    sens_dev = rows.shape[1]
    depth = kernel_hbm.shape[1]
    padded = left_mat.shape[1] // 2
    keep = probes // senses
    slot = inner.shape[1]
    width = 2 * LANES
    cols = scale.shape[1]
    count = len(chunks)
    has_left = k > 0
    has_right = k < params - 1
    has_under = s > 0
    has_over = s < senses - 1
    outer = jnp.logical_or(s == 0, s == senses - 1)
    within = jnp.logical_not(outer)
    second = lax.rem(k, 2) == 1
    first = jnp.logical_not(second)
    pair = s + 1 - 2 * lax.rem(s, 2)
    across = senses - 1 - s
    other = senses - 1 - pair

    def freq_peer(d):
        return lax.rem(f + d, groups)

    def tell(sem, **where):
        pl.semaphore_signal(sem, inc=1, device_id=where, device_id_type=MESH)

    small = [
        pltpu.make_async_copy(series_hbm, rows, small_sem.at[0]),
        pltpu.make_async_copy(short_hbm, short, small_sem.at[1]),
        pltpu.make_async_copy(tabs_hbm.at[f], tabs, small_sem.at[2]),
        pltpu.make_async_copy(prior_hbm, prior, small_sem.at[3]),
        pltpu.make_async_copy(scale_hbm, scale, small_sem.at[4]),
        pltpu.make_async_copy(img_hbm.at[f], img_tab, small_sem.at[5]),
    ]
    for copy in small:
        copy.start()

    barrier = pltpu.get_barrier_semaphore()
    for d in range(1, groups):
        tell(barrier, freq=freq_peer(d))

    @pl.when(has_under)
    def _():
        tell(barrier, sens=s - 1)

    @pl.when(has_over)
    def _():
        tell(barrier, sens=s + 1)

    @pl.when(has_left)
    def _():
        tell(barrier, param=k - 1)

    @pl.when(has_right)
    def _():
        tell(barrier, param=k + 1)

    row = lax.broadcasted_iota(jnp.int32, spread.shape, 0)
    lane = lax.broadcasted_iota(jnp.int32, spread.shape, 1)
    spread[...] = jnp.where(lane // bins_dev == row, 1.0, 0.0).astype(BF16)
    for buf in kbufs:
        pad = jnp.zeros((padded - depth, buf.shape[1]), BF16)
        buf[depth:padded] = pad
        buf[padded + depth :] = pad

    small[0].wait()
    small[1].wait()
    loads = [
        [
            pltpu.make_async_copy(
                kernel_hbm.at[part, :, pl.ds(at, width)],
                kbufs[c].at[pl.ds(part * padded, depth)],
                k_sem.at[c],
            )
            for part in range(2)
        ]
        for c, at in enumerate(chunks)
    ]
    for group in loads:
        for copy in group:
            copy.start()

    series = rows[...]

    def shortened(g):
        return jnp.dot(short[g, 0], series, preferred_element_type=F32) + jnp.dot(
            short[g, 1], series, preferred_element_type=F32
        )

    main = sens_dev // LANES * LANES
    rest = sens_dev - main
    tall_rows = squeeze * probes
    fit = LANES // rest

    def fold(part):
        lines = [part[i : i + PAIR] for i in range(0, tall_rows, PAIR)]
        folded = []
        for i in range(0, len(lines), fit):
            some = lines[i : i + fit]
            gap = jnp.zeros((PAIR, LANES - rest * len(some)), F32)
            folded.append(jnp.concatenate(some + [gap], axis=1))
        return folded

    def unfold(packed):
        parts = []
        for i in range(tall_rows // PAIR):
            line = packed[i // fit * PAIR : (i // fit + 1) * PAIR]
            parts.append(line[:, i % fit * rest : (i % fit + 1) * rest])
        return jnp.concatenate(parts, axis=0)

    for d in range(1, groups):
        g = freq_peer(d)
        value = shortened(g)
        wide = [value[:, i : i + LANES] for i in range(0, main, LANES)]
        squeezed[g] = jnp.concatenate(wide + fold(value[:, main:]), axis=0).astype(BF16)

    beside = [has_under, has_over, has_left, has_right]
    pl.semaphore_wait(barrier, groups - 1 + sum(jnp.where(b, 1, 0) for b in beside))

    def series_copy(target, slot):
        return pltpu.make_async_remote_copy(
            src_ref=squeezed.at[target],
            dst_ref=arrived.at[slot],
            send_sem=g_send,
            recv_sem=g_recv,
            device_id={"freq": target},
            device_id_type=MESH,
        )

    for d in range(1, groups):
        series_copy(freq_peer(d), f).start()
    for d in range(1, groups):
        tell(ready_x, freq=freq_peer(d))

    @pl.when(within)
    def _():
        tell(ready_z, sens=s - 1)
        tell(ready_z, sens=s + 1)

    for copy in small[2:]:
        copy.wait()
    norm = 1.0 / math.sqrt(bins_dev * groups)
    lane = lax.broadcasted_iota(jnp.int32, (8, STEP), 1) % bins_dev
    value = jnp.zeros((8, STEP), F32)
    for b in range(bins_dev):
        value = jnp.where(lane == b, prior[b] * norm, value)
    base = groups * 2 * squeeze
    for q in range(2):
        inner[q] = tabs[base + q * slot : base + (q + 1) * slot] * value[:1]

    cuts = [(at, min(STEP, padded - at)) for at in range(0, padded, STEP)]

    def expand(parts, at, span):
        first = at // bins_dev // LANES
        rows_of = spread[first * LANES : min((first + 1) * LANES, sens_dev), at : at + span]
        return jnp.dot(parts[first], rows_of, preferred_element_type=F32)

    def weighed(full, d, q, span):
        total = None
        for j in range(squeeze):
            at = (d * 2 + q) * squeeze + j
            term = full[j * probes : (j + 1) * probes] * tabs[at : at + 1, :span]
            total = term if total is None else total + term
        return total

    mine = shortened(f)
    high = mine.astype(BF16)
    low = (mine - high.astype(F32)).astype(BF16)
    mine = jnp.concatenate([high, low], axis=0)
    mine_parts = [mine[:, i : min(i + LANES, sens_dev)] for i in range(0, sens_dev, LANES)]
    for at, span in cuts:
        full = expand(mine_parts, at, span)
        full = full[: squeeze * probes] + full[squeeze * probes :]
        for q in range(2):
            ebuf[q, :, at : at + span] = weighed(full, 0, q, span)

    pl.semaphore_wait(ready_z, 1)

    @pl.when(within)
    def _():
        tell(ready_far, sens=pair)

    def loaded(c):
        part = kbufs[c].at[pl.ds(0, 2 * depth)]
        pltpu.make_async_copy(part, part, k_sem.at[c]).wait()

    loaded(0)

    def series_done():
        return pltpu.make_async_remote_copy(
            src_ref=squeezed.at[pl.ds(0, groups - 1)],
            dst_ref=arrived.at[pl.ds(0, groups - 1)],
            send_sem=g_send,
            recv_sem=g_recv,
            device_id={"freq": freq_peer(1)},
            device_id_type=MESH,
        )

    @pl.when(within)
    def _():
        for c in range(count):
            if c not in direct:
                rbuf[other, c] = jnp.zeros(rbuf.shape[2:], BF16)

    series_done().wait_recv()
    came = []
    for d in range(1, groups):
        got = arrived.at[freq_peer(d)]
        parts = [got[i * tall_rows : (i + 1) * tall_rows] for i in range(main // LANES)]
        tail = got[main // LANES * tall_rows :].astype(F32)
        came.append(parts + [unfold(tail).astype(BF16)])
    head = None
    for group in [cuts[i : i + 2] for i in range(0, len(cuts), 2)]:
        for at, span in group:
            cut = slice(at, at + span)
            fulls = [expand(c, at, span) for c in came]
            for q in range(2):
                total = ebuf[q, :, cut]
                for d in range(1, groups):
                    total = total + weighed(fulls[d - 1], d, q, span)
                ebuf[q, :, cut] = total
            which = lax.broadcasted_iota(jnp.int32, (8, span), 0) % keep
            for j in range(senses):
                both = []
                for q in range(2):
                    e = jnp.broadcast_to(ebuf[q, j * keep : j * keep + 1, cut], (8, span))
                    for r in range(1, keep):
                        here = j * keep + r
                        e = jnp.where(which == r, ebuf[q, here : here + 1, cut], e)
                    both.append(jnp.concatenate([e] * (slot // 8), axis=0))
                re, im = both
                one, two = inner[0, :, :span], inner[1, :, :span]
                block = slice(j * slot, (j + 1) * slot)
                left_mat[block, cut] = (one * re + two * im).astype(BF16)
                left_mat[block, padded + at : padded + at + span] = (one * im - two * re).astype(BF16)
        start, stop = group[0][0], group[-1][0] + group[-1][1]
        for base in (0, padded):
            term = jnp.dot(
                left_mat[:, base + start : base + stop],
                kbufs[0][base + start : base + stop],
                preferred_element_type=F32,
            )
            head = term if head is None else head + term

    def remote(src, dst, send, recv, **where):
        return pltpu.make_async_remote_copy(
            src_ref=src,
            dst_ref=dst,
            send_sem=send,
            recv_sem=recv,
            device_id=where,
            device_id_type=MESH,
        )

    def z_copy(target, c):
        return remote(
            sbuf.at[target, c], rbuf.at[s, c], z_send, z_recv.at[c], sens=target
        )

    def z_done(units, c):
        part = rbuf.at[pl.ds(0, units), c]
        return remote(part, part, z_send, z_recv.at[c], sens=pair)

    def relay_copy(c):
        return remote(
            sbuf.at[other, c], relay.at[c], z_send, relay_recv.at[c], sens=pair
        )

    def joined_copy(c):
        return remote(
            joined.at[c], rbuf.at[s, c], z_send, z_recv.at[c], sens=across
        )

    def send_sums(c):
        if c in direct:
            for target in (across, other, pair):
                z_copy(target, c).start()
            return

        @pl.when(outer)
        def _():
            z_copy(across, c).start()
            relay_copy(c).start()
            z_copy(pair, c).start()

        @pl.when(within)
        def _():
            z_copy(other, c).start()
            z_copy(pair, c).start()

    def pass_on(c):
        if c in direct:
            return

        @pl.when(within)
        def _():
            relay_copy(c).wait_recv()
            both = sbuf[across, c].astype(F32) + relay[c].astype(F32)
            joined[c] = both.astype(BF16)
            joined_copy(c).start()

    def collect(c):
        if c in direct:
            z_done(3, c).wait_recv()
        else:

            @pl.when(outer)
            def _():
                z_done(3, c).wait_recv()

            @pl.when(within)
            def _():
                z_done(2, c).wait_recv()

        total = sbuf[s, c].astype(F32)
        for slot in (pair, other, across):
            total = total + rbuf[slot, c].astype(F32)
        return total

    whole = each // 8 * 8
    for c in range(count):
        if c > 0:
            loaded(c)
        total = head
        if c > 0:
            total = jnp.dot(left_mat[...], kbufs[c][...], preferred_element_type=F32)
        for j in range(senses):
            halves = [
                total[j * slot : (j + 1) * slot, h * LANES : (h + 1) * LANES] for h in range(2)
            ]
            packed = [half[:whole] for half in halves]
            if slot > each:
                packed.append(halves[0][whole:] + pltpu.roll(halves[1][whole:], each - whole, 0))
            sbuf[j, c] = jnp.concatenate(packed, axis=0).astype(BF16)
        if c == 0:

            @pl.when(outer)
            def _():
                pl.semaphore_wait(ready_far, 1)

        send_sums(c)

    def x_copy(target, c):
        part = gath.at[f, c]
        return remote(part, part, x_send, x_recv.at[c], freq=target)

    def x_done(c):
        part = gath.at[pl.ds(0, groups - 1), c]
        return remote(part, part, x_send, x_recv.at[c], freq=freq_peer(1))

    def to_left(target):
        return remote(
            edges.at[0],
            halo_right.at[f],
            hl_send,
            hr_recv,
            freq=target,
            param=jnp.maximum(k - 1, 0),
        )

    def to_right(target):
        return remote(
            edges.at[1],
            halo_left.at[f],
            hr_send,
            hl_recv,
            freq=target,
            param=jnp.minimum(k + 1, params - 1),
        )

    rows_out = scaled.shape[0]
    tall = img_tab.shape[1] // 2

    def image_of(pieces):
        total = None
        for index, piece in pieces:
            term = jnp.dot(img_tab[index], piece, preferred_element_type=F32)
            total = term if total is None else total + term
        return total[:rows_out], total[tall : tall + rows_out]

    def twice(g, piece):
        return [(g, piece), (groups + g, piece)]

    def begin(c):
        pieces = twice(f, gath[f, c]) + [(2 * groups, lows[c])]
        for half, image in enumerate(image_of(pieces)):
            at = chunks[c] + half * LANES
            scaled[:, at : at + LANES] = image

    def finish(c):
        x_done(c).wait_recv()
        pieces = []
        for d in range(1, groups):
            pieces += twice(freq_peer(d), gath[freq_peer(d), c])
        for half, image in enumerate(image_of(pieces)):
            at = chunks[c] + half * LANES
            lanes = slice(at, at + LANES)
            scaled[:, lanes] = (scaled[:, lanes] + image) * scale[:, lanes]

    pl.semaphore_wait(ready_x, groups - 1)
    for c in range(count):
        pass_on(c)
    for c, at in enumerate(chunks):
        total = collect(c)
        high = total.astype(BF16)
        gath[f, c] = high
        for d in range(1, groups):
            x_copy(freq_peer(d), c).start()
        lows[c] = (total - high.astype(F32)).astype(BF16)
        if at == 0:
            edges[0] = (total * scale[:, :LANES]).astype(BF16)

            @pl.when(has_left)
            def _():
                for d in range(groups):
                    to_left(freq_peer(d)).start()

        if at + width == cols:
            edges[1] = (total * scale[:, cols - LANES :]).astype(BF16)

            @pl.when(has_right)
            def _():
                for d in range(groups):
                    to_right(freq_peer(d)).start()

    for c in range(count):
        begin(c)

    def halo_done(ref, send, recv):
        return remote(ref, ref, send, recv, freq=freq_peer(1))

    @pl.when(has_left)
    def _():
        halo_done(halo_left, hr_send, hl_recv).wait_recv()

    @pl.when(jnp.logical_not(has_left))
    def _():
        halo_left[...] = jnp.zeros_like(halo_left)

    @pl.when(has_right)
    def _():
        halo_done(halo_right, hl_send, hr_recv).wait_recv()

    @pl.when(jnp.logical_not(has_right))
    def _():
        halo_right[...] = jnp.zeros_like(halo_right)

    _, left = image_of(sum([twice(g, halo_left[g]) for g in range(groups)], []))
    right, _ = image_of(sum([twice(g, halo_right[g]) for g in range(groups)], []))
    for c in range(count - 1):
        finish(c)

    def smooth(at, end):
        if at >= end:
            return
        mid = scaled[:, at:end]
        before = scaled[:, at - 1 : at] if at > 0 else left[:, LANES - 1 :]
        after = scaled[:, end : end + 1] if end < cols else right[:, :1]
        lower = jnp.concatenate([before, mid[:, :-1]], axis=1)
        upper = jnp.concatenate([mid[:, 1:], after], axis=1)
        value = scale[:, at:end] * (0.5 * mid + 0.25 * (lower + upper))
        out_ref[:, :, at:end] = value.reshape(out_ref.shape[0], keep, end - at)

    at = chunks[-1]
    start, stop = max(at - LANES, 0), min(at + width + LANES, cols)
    smooth(0, start)
    smooth(stop, cols)
    finish(count - 1)
    smooth(start, stop)

    series_done().wait_send()
    part = sbuf.at[pl.ds(0, 3)]
    remote(part, part, z_send, z_recv.at[0], sens=pair).wait_send()
    part = gath.at[pl.ds(0, groups - 1)]
    remote(part, part, x_send, x_recv.at[0], freq=freq_peer(1)).wait_send()

    @pl.when(has_left)
    def _():
        halo_done(halo_right, hl_send, hr_recv).wait_send()

    @pl.when(has_right)
    def _():
        halo_done(halo_left, hr_send, hl_recv).wait_send()


def local(mesh_shape, series, kernel, prior_spectrum, prior_scale):
    groups, params, senses = (mesh_shape[n] for n in ("freq", "param", "sens"))
    assert senses == 4 and groups > 1
    probes, sens_dev, time_dev = series.shape
    _, bins_dev, _, cols = kernel.shape
    keep = probes // senses
    width = 2 * LANES
    assert cols % width == 0
    chunks = list(range(0, cols, width))
    chunks = chunks[:1] + chunks[:0:-1][:1] + chunks[1:-1]
    direct = (len(chunks) - 1,)
    count = len(chunks)
    depth = sens_dev * bins_dev
    padded = -(-depth // LANES) * LANES
    short, long, squeeze = series_tables(groups, bins_dev, time_dev, probes)
    img_tab, inner, each, slot = image_tables(groups, bins_dev, time_dev, keep)
    tabs = np.concatenate([long, inner], axis=1)
    main = sens_dev // LANES
    fit = LANES // (sens_dev - main * LANES)
    assert squeeze * probes % PAIR == 0
    lines = main * squeeze * probes + -(-squeeze * probes // PAIR // fit) * PAIR
    tabs = np.tile(tabs, (1, 1, STEP // bins_dev)).astype(np.float32)
    unit = (2 * each, LANES)
    dma = pltpu.SemaphoreType.DMA
    plain = pltpu.SemaphoreType.REGULAR
    return pl.pallas_call(
        functools.partial(
            body, (groups, params, senses, chunks, direct, bins_dev, probes, squeeze, each)
        ),
        out_shape=pltpu.VMEM((time_dev, keep, cols), F32),
        in_specs=[pl.BlockSpec(memory_space=pltpu.HBM)] * 7,
        out_specs=pl.BlockSpec(memory_space=pltpu.VMEM),
        scratch_shapes=[
            [pltpu.VMEM((2 * padded, width), BF16) for _ in chunks],
            pltpu.VMEM((time_dev * probes, sens_dev), BF16),
            pltpu.SMEM((bins_dev,), F32),
            pltpu.VMEM((1, cols), F32),
            pltpu.VMEM(short.shape, BF16),
            pltpu.VMEM(tabs.shape[1:], F32),
            pltpu.VMEM(img_tab.shape[1:], BF16),
            pltpu.VMEM((2, slot, STEP), F32),
            pltpu.VMEM((groups, lines, LANES), BF16),
            pltpu.VMEM((groups, lines, LANES), BF16),
            pltpu.VMEM((sens_dev, padded), BF16),
            pltpu.VMEM((2, probes, padded), F32),
            pltpu.VMEM((senses * slot, 2 * padded), BF16),
            pltpu.VMEM((senses, count) + unit, BF16),
            pltpu.VMEM((senses, count) + unit, BF16),
            pltpu.VMEM((count,) + unit, BF16),
            pltpu.VMEM((count,) + unit, BF16),
            pltpu.VMEM((groups, count) + unit, BF16),
            pltpu.VMEM((count,) + unit, BF16),
            pltpu.VMEM((time_dev * keep, cols), F32),
            pltpu.VMEM((2,) + unit, BF16),
            pltpu.VMEM((groups,) + unit, BF16),
            pltpu.VMEM((groups,) + unit, BF16),
            dma((6,)),
            dma((count,)),
            dma,
            dma,
            dma,
            dma((count,)),
            dma((count,)),
            dma,
            dma((count,)),
            dma,
            dma,
            dma,
            dma,
            plain,
            plain,
            plain,
        ],
        compiler_params=pltpu.CompilerParams(
            collective_id=0, has_side_effects=True, vmem_limit_bytes=60 * 1024 * 1024
        ),
    )(
        series.transpose(2, 0, 1).reshape(time_dev * probes, sens_dev),
        kernel.transpose(0, 2, 1, 3).reshape(2, depth, cols),
        prior_spectrum,
        prior_scale.reshape(1, cols),
        jnp.asarray(short),
        jnp.asarray(tabs),
        jnp.asarray(img_tab),
    )


def solution(mesh):
    placed = (P(None, "sens", "freq"), P(None, "freq", "sens", "param"), P("freq"), P("param"))
    return jax.shard_map(
        functools.partial(local, dict(mesh.shape)),
        mesh=mesh,
        in_specs=placed,
        out_specs=P("freq", "sens", "param"),
        check_vma=False,
    )
```

```python
import functools
import math

import jax
import jax.numpy as jnp
import numpy as np
from jax import lax
from jax.experimental import pallas as pl
from jax.experimental.pallas import tpu as pltpu
from jax.sharding import PartitionSpec as P

LEN = 840
MESH = pl.DeviceIdType.MESH
BF16 = jnp.bfloat16
F32 = jnp.float32
RESIDUAL = 2.0**-26
STEP = 256
LANES = 128
PAIR = 16


def split(table):
    table = table.astype(np.float32)
    high = table.astype(BF16)
    low = (table - high.astype(np.float32)).astype(BF16)
    return high, low


def phases(groups, bins_dev, time_dev):
    bins, times = groups * bins_dev, groups * time_dev
    angle = 2.0 * np.pi * ((np.arange(times)[:, None] * np.arange(bins)[None, :]) % LEN) / LEN
    both = np.stack([np.cos(angle), -np.sin(angle)], axis=1)
    both = both.reshape(times, 2, groups, bins_dev).transpose(2, 0, 1, 3)
    return both.reshape(groups, times, 2 * bins_dev)


def factor(table, multiple):
    left, size, right = np.linalg.svd(table, full_matrices=False)
    rank = size.size
    for r in range(1, size.size):
        if np.abs(table - (left[:, :r] * size[:r]) @ right[:r]).max() < RESIDUAL:
            rank = r
            break
    rank = min(-(-rank // multiple) * multiple, size.size)
    return left * size, right, rank


def with_probes(table, probes):
    full = np.einsum("...ij,qr->...iqjr", table, np.eye(probes))
    lead = table.shape[:-2]
    return full.reshape(lead + (table.shape[-2] * probes, table.shape[-1] * probes))


def series_tables(groups, bins_dev, time_dev, probes):
    comps = phases(groups, bins_dev, time_dev) / math.sqrt(groups * time_dev)
    blocks = comps.reshape(groups, groups, time_dev, 2 * bins_dev).transpose(0, 1, 3, 2)
    parts = [factor(block.reshape(-1, time_dev), 2) for block in blocks]
    rank = max(part[2] for part in parts)
    short = np.stack([right[:rank] for _, right, _ in parts])
    short = np.concatenate(split(with_probes(short, probes)), axis=1)
    long = np.stack([left[:, :rank] for left, _, _ in parts])
    long = long.reshape(groups, groups, 2, bins_dev, rank).transpose(0, 1, 2, 4, 3)
    long = np.stack([np.roll(long[g], -g, axis=0) for g in range(groups)])
    return short, long.reshape(groups, -1, bins_dev), rank


def packing(each):
    whole = each // 8 * 8
    first = np.concatenate([np.arange(whole), 2 * whole + np.arange(each - whole)])
    second = np.concatenate([whole + np.arange(whole), whole + each + np.arange(each - whole)])
    return first, second


def image_tables(groups, bins_dev, time_dev, keep):
    comps = phases(groups, bins_dev, time_dev)
    parts = [factor(comp, 2) for comp in comps]
    rank = max(part[2] for part in parts)
    each, rows = rank * keep, time_dev * keep
    outer = np.stack([left[:, :rank] for left, _, _ in parts])
    outer = outer.reshape(groups, groups, time_dev, rank).transpose(1, 0, 2, 3)
    full = np.einsum("ghtj,qr->ghtqjr", outer, np.eye(keep))
    full = full.reshape(groups, groups, rows, each)
    tall = -(-rows // 8) * 8
    packed = np.zeros((groups, groups, 2 * tall, 2 * each))
    for half, places in enumerate(packing(each)):
        packed[:, :, half * tall : half * tall + rows, places] = full
    high, low = split(packed)
    image = np.concatenate([high, low], axis=2)
    inner = np.stack([right[:rank] for _, right, _ in parts])
    inner = inner.reshape(groups, rank, 2, bins_dev).transpose(0, 2, 1, 3)
    inner = np.repeat(inner, keep, axis=2)
    slot = -(-each // 8) * 8
    inner = np.pad(inner, ((0, 0), (0, 0), (0, slot - each), (0, 0)))
    return image, inner.reshape(groups, -1, bins_dev), each, slot


def body(
    cfg,
    series_hbm,
    kernel_hbm,
    prior_hbm,
    scale_hbm,
    short_hbm,
    tabs_hbm,
    img_hbm,
    out_ref,
    kbufs,
    rows,
    prior,
    scale,
    short,
    tabs,
    img_tab,
    inner,
    squeezed,
    arrived,
    spread,
    ebuf,
    left_mat,
    sbuf,
    rbuf,
    relay,
    joined,
    gath,
    lows,
    scaled,
    edges,
    halo_left,
    halo_right,
    small_sem,
    k_sem,
    g_send,
    g_recv,
    z_send,
    z_recv,
    relay_recv,
    x_send,
    x_recv,
    hl_send,
    hl_recv,
    hr_send,
    hr_recv,
    ready_x,
    ready_z,
    ready_far,
):
    groups, params, senses, chunks, joint, direct, bins_dev, probes, squeeze, each = cfg
    f = lax.axis_index("freq")
    k = lax.axis_index("param")
    s = lax.axis_index("sens")
    sens_dev = rows.shape[1]
    depth = kernel_hbm.shape[1]
    padded = left_mat.shape[1] // 2
    keep = probes // senses
    slot = inner.shape[1]
    width = 2 * LANES
    cols = scale.shape[1]
    count = len(chunks)
    has_left = k > 0
    has_right = k < params - 1
    has_under = s > 0
    has_over = s < senses - 1
    outer = jnp.logical_or(s == 0, s == senses - 1)
    within = jnp.logical_not(outer)
    second = lax.rem(k, 2) == 1
    first = jnp.logical_not(second)
    pair = s + 1 - 2 * lax.rem(s, 2)
    across = senses - 1 - s
    other = senses - 1 - pair

    def freq_peer(d):
        return lax.rem(f + d, groups)

    def tell(sem, **where):
        pl.semaphore_signal(sem, inc=1, device_id=where, device_id_type=MESH)

    small = [
        pltpu.make_async_copy(series_hbm, rows, small_sem.at[0]),
        pltpu.make_async_copy(short_hbm, short, small_sem.at[1]),
        pltpu.make_async_copy(tabs_hbm.at[f], tabs, small_sem.at[2]),
        pltpu.make_async_copy(prior_hbm, prior, small_sem.at[3]),
        pltpu.make_async_copy(scale_hbm, scale, small_sem.at[4]),
        pltpu.make_async_copy(img_hbm.at[f], img_tab, small_sem.at[5]),
    ]
    for copy in small:
        copy.start()

    barrier = pltpu.get_barrier_semaphore()
    for d in range(1, groups):
        tell(barrier, freq=freq_peer(d))

    @pl.when(has_under)
    def _():
        tell(barrier, sens=s - 1)

    @pl.when(has_over)
    def _():
        tell(barrier, sens=s + 1)

    @pl.when(has_left)
    def _():
        tell(barrier, param=k - 1)

    @pl.when(has_right)
    def _():
        tell(barrier, param=k + 1)

    row = lax.broadcasted_iota(jnp.int32, spread.shape, 0)
    lane = lax.broadcasted_iota(jnp.int32, spread.shape, 1)
    spread[...] = jnp.where(lane // bins_dev == row, 1.0, 0.0).astype(BF16)
    for buf in kbufs:
        pad = jnp.zeros((padded - depth, buf.shape[1]), BF16)
        buf[depth:padded] = pad
        buf[padded + depth :] = pad

    small[0].wait()
    small[1].wait()
    loads = [
        [
            pltpu.make_async_copy(
                kernel_hbm.at[part, :, pl.ds(chunks[c], width)],
                kbufs[i].at[pl.ds(part * padded, depth), pl.ds(n * width, width)],
                k_sem.at[i],
            )
            for n, c in enumerate(some)
            for part in range(2)
        ]
        for i, some in enumerate(joint)
    ]
    for group in loads:
        for copy in group:
            copy.start()

    series = rows[...]

    def shortened(g):
        both = jnp.dot(short[g], series, preferred_element_type=F32)
        return both[: squeeze * probes] + both[squeeze * probes :]

    main = sens_dev // LANES * LANES
    rest = sens_dev - main
    tall_rows = squeeze * probes
    fit = LANES // rest

    def fold(part):
        lines = [part[i : i + PAIR] for i in range(0, tall_rows, PAIR)]
        folded = []
        for i in range(0, len(lines), fit):
            some = lines[i : i + fit]
            gap = jnp.zeros((PAIR, LANES - rest * len(some)), F32)
            folded.append(jnp.concatenate(some + [gap], axis=1))
        return folded

    def unfold(packed):
        parts = []
        for i in range(tall_rows // PAIR):
            line = packed[i // fit * PAIR : (i // fit + 1) * PAIR]
            parts.append(line[:, i % fit * rest : (i % fit + 1) * rest])
        return jnp.concatenate(parts, axis=0)

    for d in range(1, groups):
        g = freq_peer(d)
        value = shortened(g)
        wide = [value[:, i : i + LANES] for i in range(0, main, LANES)]
        squeezed[g] = jnp.concatenate(wide + fold(value[:, main:]), axis=0).astype(BF16)

    beside = [has_under, has_over, has_left, has_right]
    pl.semaphore_wait(barrier, groups - 1 + sum(jnp.where(b, 1, 0) for b in beside))

    def series_copy(target, slot):
        return pltpu.make_async_remote_copy(
            src_ref=squeezed.at[target],
            dst_ref=arrived.at[slot],
            send_sem=g_send,
            recv_sem=g_recv,
            device_id={"freq": target},
            device_id_type=MESH,
        )

    for d in range(1, groups):
        series_copy(freq_peer(d), f).start()
    for d in range(1, groups):
        tell(ready_x, freq=freq_peer(d))

    @pl.when(within)
    def _():
        tell(ready_z, sens=s - 1)
        tell(ready_z, sens=s + 1)

    for copy in small[2:]:
        copy.wait()
    norm = 1.0 / math.sqrt(bins_dev * groups)
    lane = lax.broadcasted_iota(jnp.int32, (8, STEP), 1) % bins_dev
    value = jnp.zeros((8, STEP), F32)
    for b in range(bins_dev):
        value = jnp.where(lane == b, prior[b] * norm, value)
    base = groups * 2 * squeeze
    for q in range(2):
        inner[q] = tabs[base + q * slot : base + (q + 1) * slot] * value[:1]

    cuts = [(at, min(STEP, padded - at)) for at in range(0, padded, STEP)]

    def expand(parts, at, span):
        first = at // bins_dev // LANES
        rows_of = spread[first * LANES : min((first + 1) * LANES, sens_dev), at : at + span]
        return jnp.dot(parts[first], rows_of, preferred_element_type=F32)

    def weighed(full, d, q, span):
        total = None
        for j in range(squeeze):
            at = (d * 2 + q) * squeeze + j
            term = full[j * probes : (j + 1) * probes] * tabs[at : at + 1, :span]
            total = term if total is None else total + term
        return total

    mine = shortened(f)
    high = mine.astype(BF16)
    low = (mine - high.astype(F32)).astype(BF16)
    mine = jnp.concatenate([high, low], axis=0)
    mine_parts = [mine[:, i : min(i + LANES, sens_dev)] for i in range(0, sens_dev, LANES)]
    for at, span in cuts:
        full = expand(mine_parts, at, span)
        full = full[: squeeze * probes] + full[squeeze * probes :]
        for q in range(2):
            ebuf[q, :, at : at + span] = weighed(full, 0, q, span)

    pl.semaphore_wait(ready_z, 1)

    @pl.when(within)
    def _():
        tell(ready_far, sens=pair)

    def loaded(i):
        part = kbufs[i].at[pl.ds(0, 2 * depth)]
        pltpu.make_async_copy(part, part, k_sem.at[i]).wait()

    loaded(0)

    def series_done():
        return pltpu.make_async_remote_copy(
            src_ref=squeezed.at[pl.ds(0, groups - 1)],
            dst_ref=arrived.at[pl.ds(0, groups - 1)],
            send_sem=g_send,
            recv_sem=g_recv,
            device_id={"freq": freq_peer(1)},
            device_id_type=MESH,
        )

    @pl.when(within)
    def _():
        for c in range(count):
            if c not in direct:
                rbuf[other, c] = jnp.zeros(rbuf.shape[2:], BF16)

    series_done().wait_recv()
    came = []
    for d in range(1, groups):
        got = arrived.at[freq_peer(d)]
        parts = [got[i * tall_rows : (i + 1) * tall_rows] for i in range(main // LANES)]
        tail = got[main // LANES * tall_rows :].astype(F32)
        came.append(parts + [unfold(tail).astype(BF16)])
    head = None
    for group in [cuts[i : i + 2] for i in range(0, len(cuts), 2)]:
        for at, span in group:
            cut = slice(at, at + span)
            fulls = [expand(c, at, span) for c in came]
            for q in range(2):
                total = ebuf[q, :, cut]
                for d in range(1, groups):
                    total = total + weighed(fulls[d - 1], d, q, span)
                ebuf[q, :, cut] = total
            which = lax.broadcasted_iota(jnp.int32, (8, span), 0) % keep
            for j in range(senses):
                both = []
                for q in range(2):
                    e = jnp.broadcast_to(ebuf[q, j * keep : j * keep + 1, cut], (8, span))
                    for r in range(1, keep):
                        here = j * keep + r
                        e = jnp.where(which == r, ebuf[q, here : here + 1, cut], e)
                    both.append(jnp.concatenate([e] * (slot // 8), axis=0))
                re, im = both
                one, two = inner[0, :, :span], inner[1, :, :span]
                block = slice(j * slot, (j + 1) * slot)
                left_mat[block, cut] = (one * re + two * im).astype(BF16)
                left_mat[block, padded + at : padded + at + span] = (one * im - two * re).astype(BF16)
        start, stop = group[0][0], group[-1][0] + group[-1][1]
        for base in (0, padded):
            term = jnp.dot(
                left_mat[:, base + start : base + stop],
                kbufs[0][base + start : base + stop],
                preferred_element_type=F32,
            )
            head = term if head is None else head + term

    def remote(src, dst, send, recv, **where):
        return pltpu.make_async_remote_copy(
            src_ref=src,
            dst_ref=dst,
            send_sem=send,
            recv_sem=recv,
            device_id=where,
            device_id_type=MESH,
        )

    def z_copy(target, c):
        return remote(
            sbuf.at[target, c], rbuf.at[s, c], z_send, z_recv.at[c], sens=target
        )

    def z_done(units, c):
        part = rbuf.at[pl.ds(0, units), c]
        return remote(part, part, z_send, z_recv.at[c], sens=pair)

    def relay_copy(c):
        return remote(
            sbuf.at[other, c], relay.at[c], z_send, relay_recv.at[c], sens=pair
        )

    def joined_copy(c):
        return remote(
            joined.at[c], rbuf.at[s, c], z_send, z_recv.at[c], sens=across
        )

    def send_sums(c):
        if c in direct:
            for target in (across, other, pair):
                z_copy(target, c).start()
            return

        @pl.when(outer)
        def _():
            z_copy(across, c).start()
            relay_copy(c).start()
            z_copy(pair, c).start()

        @pl.when(within)
        def _():
            z_copy(other, c).start()
            z_copy(pair, c).start()

    def pass_on(c):
        if c in direct:
            return

        @pl.when(within)
        def _():
            relay_copy(c).wait_recv()
            both = sbuf[across, c].astype(F32) + relay[c].astype(F32)
            joined[c] = both.astype(BF16)
            joined_copy(c).start()

    def collect(c):
        if c in direct:
            z_done(3, c).wait_recv()
        else:

            @pl.when(outer)
            def _():
                z_done(3, c).wait_recv()

            @pl.when(within)
            def _():
                z_done(2, c).wait_recv()

        total = sbuf[s, c].astype(F32)
        for slot in (pair, other, across):
            total = total + rbuf[slot, c].astype(F32)
        return total

    whole = each // 8 * 8
    for i, some in enumerate(joint):
        total = head
        if i > 0:
            loaded(i)
            total = jnp.dot(left_mat[...], kbufs[i][...], preferred_element_type=F32)
        for n, c in enumerate(some):
            for j in range(senses):
                block = total[j * slot : (j + 1) * slot, n * width : (n + 1) * width]
                halves = [block[:, h * LANES : (h + 1) * LANES] for h in range(2)]
                packed = [half[:whole] for half in halves]
                if slot > each:
                    turned = pltpu.roll(halves[1][whole:], each - whole, 0)
                    packed.append(halves[0][whole:] + turned)
                sbuf[j, c] = jnp.concatenate(packed, axis=0).astype(BF16)
        if i == 0:

            @pl.when(outer)
            def _():
                pl.semaphore_wait(ready_far, 1)

        for c in some:
            send_sums(c)

    def x_copy(target, c):
        part = gath.at[f, c]
        return remote(part, part, x_send, x_recv.at[c], freq=target)

    def x_done(c):
        part = gath.at[pl.ds(0, groups - 1), c]
        return remote(part, part, x_send, x_recv.at[c], freq=freq_peer(1))

    def to_left(target):
        return remote(
            edges.at[0],
            halo_right.at[f],
            hl_send,
            hr_recv,
            freq=target,
            param=jnp.maximum(k - 1, 0),
        )

    def to_right(target):
        return remote(
            edges.at[1],
            halo_left.at[f],
            hr_send,
            hl_recv,
            freq=target,
            param=jnp.minimum(k + 1, params - 1),
        )

    rows_out = scaled.shape[0]
    tall = img_tab.shape[1] // 4

    def image_of(pieces, lower=None):
        total = None
        for g, piece in pieces:
            term = jnp.dot(img_tab[g], piece, preferred_element_type=F32)
            total = term if total is None else total + term
        total = total[: 2 * tall] + total[2 * tall :]
        if lower is not None:
            total = total + jnp.dot(img_tab[f, : 2 * tall], lower, preferred_element_type=F32)
        return total[:rows_out], total[tall : tall + rows_out]

    def begin(c):
        for half, image in enumerate(image_of([(f, gath[f, c])], lows[c])):
            at = chunks[c] + half * LANES
            scaled[:, at : at + LANES] = image

    def finish(c):
        x_done(c).wait_recv()
        pieces = [(freq_peer(d), gath[freq_peer(d), c]) for d in range(1, groups)]
        for half, image in enumerate(image_of(pieces)):
            at = chunks[c] + half * LANES
            lanes = slice(at, at + LANES)
            scaled[:, lanes] = (scaled[:, lanes] + image) * scale[:, lanes]

    pl.semaphore_wait(ready_x, groups - 1)
    for c in range(count):
        pass_on(c)
    for c, at in enumerate(chunks):
        total = collect(c)
        high = total.astype(BF16)
        gath[f, c] = high
        for d in range(1, groups):
            x_copy(freq_peer(d), c).start()
        lows[c] = (total - high.astype(F32)).astype(BF16)
        if at == 0:
            edges[0] = (total * scale[:, :LANES]).astype(BF16)

            @pl.when(has_left)
            def _():
                for d in range(groups):
                    to_left(freq_peer(d)).start()

        if at + width == cols:
            edges[1] = (total * scale[:, cols - LANES :]).astype(BF16)

            @pl.when(has_right)
            def _():
                for d in range(groups):
                    to_right(freq_peer(d)).start()

    for c in range(count):
        begin(c)

    def halo_done(ref, send, recv):
        return remote(ref, ref, send, recv, freq=freq_peer(1))

    @pl.when(has_left)
    def _():
        halo_done(halo_left, hr_send, hl_recv).wait_recv()

    @pl.when(jnp.logical_not(has_left))
    def _():
        halo_left[...] = jnp.zeros_like(halo_left)

    @pl.when(has_right)
    def _():
        halo_done(halo_right, hl_send, hr_recv).wait_recv()

    @pl.when(jnp.logical_not(has_right))
    def _():
        halo_right[...] = jnp.zeros_like(halo_right)

    _, left = image_of([(g, halo_left[g]) for g in range(groups)])
    right, _ = image_of([(g, halo_right[g]) for g in range(groups)])
    for c in range(count - 1):
        finish(c)

    def smooth(at, end):
        if at >= end:
            return
        mid = scaled[:, at:end]
        before = scaled[:, at - 1 : at] if at > 0 else left[:, LANES - 1 :]
        after = scaled[:, end : end + 1] if end < cols else right[:, :1]
        lower = jnp.concatenate([before, mid[:, :-1]], axis=1)
        upper = jnp.concatenate([mid[:, 1:], after], axis=1)
        value = scale[:, at:end] * (0.5 * mid + 0.25 * (lower + upper))
        out_ref[:, :, at:end] = value.reshape(out_ref.shape[0], keep, end - at)

    at = chunks[-1]
    start, stop = max(at - LANES, 0), min(at + width + LANES, cols)
    smooth(0, start)
    smooth(stop, cols)
    finish(count - 1)
    smooth(start, stop)

    series_done().wait_send()
    part = sbuf.at[pl.ds(0, 3)]
    remote(part, part, z_send, z_recv.at[0], sens=pair).wait_send()
    part = gath.at[pl.ds(0, groups - 1)]
    remote(part, part, x_send, x_recv.at[0], freq=freq_peer(1)).wait_send()

    @pl.when(has_left)
    def _():
        halo_done(halo_right, hl_send, hr_recv).wait_send()

    @pl.when(has_right)
    def _():
        halo_done(halo_left, hr_send, hl_recv).wait_send()


def local(mesh_shape, series, kernel, prior_spectrum, prior_scale):
    groups, params, senses = (mesh_shape[n] for n in ("freq", "param", "sens"))
    assert senses == 4 and groups > 1
    probes, sens_dev, time_dev = series.shape
    _, bins_dev, _, cols = kernel.shape
    keep = probes // senses
    width = 2 * LANES
    assert cols % width == 0
    chunks = list(range(0, cols, width))
    chunks = chunks[:1] + chunks[:0:-1][:1] + chunks[1:-1]
    direct = tuple(range(len(chunks) // 2, len(chunks)))
    joint = [[0], list(range(1, len(chunks) - 1)), [len(chunks) - 1]]
    count = len(chunks)
    depth = sens_dev * bins_dev
    padded = -(-depth // LANES) * LANES
    short, long, squeeze = series_tables(groups, bins_dev, time_dev, probes)
    img_tab, inner, each, slot = image_tables(groups, bins_dev, time_dev, keep)
    tabs = np.concatenate([long, inner], axis=1)
    main = sens_dev // LANES
    fit = LANES // (sens_dev - main * LANES)
    assert squeeze * probes % PAIR == 0
    lines = main * squeeze * probes + -(-squeeze * probes // PAIR // fit) * PAIR
    tabs = np.tile(tabs, (1, 1, STEP // bins_dev)).astype(np.float32)
    unit = (2 * each, LANES)
    dma = pltpu.SemaphoreType.DMA
    plain = pltpu.SemaphoreType.REGULAR
    return pl.pallas_call(
        functools.partial(
            body, (groups, params, senses, chunks, joint, direct, bins_dev, probes, squeeze, each)
        ),
        out_shape=pltpu.VMEM((time_dev, keep, cols), F32),
        in_specs=[pl.BlockSpec(memory_space=pltpu.HBM)] * 7,
        out_specs=pl.BlockSpec(memory_space=pltpu.VMEM),
        scratch_shapes=[
            [pltpu.VMEM((2 * padded, width * len(some)), BF16) for some in joint],
            pltpu.VMEM((time_dev * probes, sens_dev), BF16),
            pltpu.SMEM((bins_dev,), F32),
            pltpu.VMEM((1, cols), F32),
            pltpu.VMEM(short.shape, BF16),
            pltpu.VMEM(tabs.shape[1:], F32),
            pltpu.VMEM(img_tab.shape[1:], BF16),
            pltpu.VMEM((2, slot, STEP), F32),
            pltpu.VMEM((groups, lines, LANES), BF16),
            pltpu.VMEM((groups, lines, LANES), BF16),
            pltpu.VMEM((sens_dev, padded), BF16),
            pltpu.VMEM((2, probes, padded), F32),
            pltpu.VMEM((senses * slot, 2 * padded), BF16),
            pltpu.VMEM((senses, count) + unit, BF16),
            pltpu.VMEM((senses, count) + unit, BF16),
            pltpu.VMEM((count,) + unit, BF16),
            pltpu.VMEM((count,) + unit, BF16),
            pltpu.VMEM((groups, count) + unit, BF16),
            pltpu.VMEM((count,) + unit, BF16),
            pltpu.VMEM((time_dev * keep, cols), F32),
            pltpu.VMEM((2,) + unit, BF16),
            pltpu.VMEM((groups,) + unit, BF16),
            pltpu.VMEM((groups,) + unit, BF16),
            dma((6,)),
            dma((len(joint),)),
            dma,
            dma,
            dma,
            dma((count,)),
            dma((count - len(direct),)),
            dma,
            dma((count,)),
            dma,
            dma,
            dma,
            dma,
            plain,
            plain,
            plain,
        ],
        compiler_params=pltpu.CompilerParams(
            collective_id=0, has_side_effects=True, vmem_limit_bytes=60 * 1024 * 1024
        ),
    )(
        series.transpose(2, 0, 1).reshape(time_dev * probes, sens_dev),
        kernel.transpose(0, 2, 1, 3).reshape(2, depth, cols),
        prior_spectrum,
        prior_scale.reshape(1, cols),
        jnp.asarray(short),
        jnp.asarray(tabs),
        jnp.asarray(img_tab),
    )


def solution(mesh):
    placed = (P(None, "sens", "freq"), P(None, "freq", "sens", "param"), P("freq"), P("param"))
    return jax.shard_map(
        functools.partial(local, dict(mesh.shape)),
        mesh=mesh,
        in_specs=placed,
        out_specs=P("freq", "sens", "param"),
        check_vma=False,
    )
```

```python
import functools
import math

import jax
import jax.numpy as jnp
import numpy as np
from jax import lax
from jax.experimental import pallas as pl
from jax.experimental.pallas import tpu as pltpu
from jax.sharding import PartitionSpec as P

LEN = 840
MESH = pl.DeviceIdType.MESH
BF16 = jnp.bfloat16
F32 = jnp.float32
RESIDUAL = 2.0**-26
STEP = 256
LANES = 128
PAIR = 16


def split(table):
    table = table.astype(np.float32)
    high = table.astype(BF16)
    low = (table - high.astype(np.float32)).astype(BF16)
    return high, low


def phases(groups, bins_dev, time_dev):
    bins, times = groups * bins_dev, groups * time_dev
    angle = 2.0 * np.pi * ((np.arange(times)[:, None] * np.arange(bins)[None, :]) % LEN) / LEN
    both = np.stack([np.cos(angle), -np.sin(angle)], axis=1)
    both = both.reshape(times, 2, groups, bins_dev).transpose(2, 0, 1, 3)
    return both.reshape(groups, times, 2 * bins_dev)


def factor(table, multiple):
    left, size, right = np.linalg.svd(table, full_matrices=False)
    rank = size.size
    for r in range(1, size.size):
        if np.abs(table - (left[:, :r] * size[:r]) @ right[:r]).max() < RESIDUAL:
            rank = r
            break
    rank = min(-(-rank // multiple) * multiple, size.size)
    return left * size, right, rank


def with_probes(table, probes):
    full = np.einsum("...ij,qr->...iqjr", table, np.eye(probes))
    lead = table.shape[:-2]
    return full.reshape(lead + (table.shape[-2] * probes, table.shape[-1] * probes))


def series_tables(groups, bins_dev, time_dev, probes):
    comps = phases(groups, bins_dev, time_dev) / math.sqrt(groups * time_dev)
    blocks = comps.reshape(groups, groups, time_dev, 2 * bins_dev).transpose(0, 1, 3, 2)
    parts = [factor(block.reshape(-1, time_dev), 2) for block in blocks]
    rank = max(part[2] for part in parts)
    short = np.stack([right[:rank] for _, right, _ in parts])
    short = np.concatenate(split(with_probes(short, probes)), axis=1)
    long = np.stack([left[:, :rank] for left, _, _ in parts])
    long = long.reshape(groups, groups, 2, bins_dev, rank).transpose(0, 1, 2, 4, 3)
    long = np.stack([np.roll(long[g], -g, axis=0) for g in range(groups)])
    return short, long.reshape(groups, -1, bins_dev), rank


def packing(each):
    whole = each // 8 * 8
    first = np.concatenate([np.arange(whole), 2 * whole + np.arange(each - whole)])
    second = np.concatenate([whole + np.arange(whole), whole + each + np.arange(each - whole)])
    return first, second


def image_tables(groups, bins_dev, time_dev, keep):
    comps = phases(groups, bins_dev, time_dev)
    parts = [factor(comp, 2) for comp in comps]
    rank = max(part[2] for part in parts)
    each, rows = rank * keep, time_dev * keep
    outer = np.stack([left[:, :rank] for left, _, _ in parts])
    outer = outer.reshape(groups, groups, time_dev, rank).transpose(1, 0, 2, 3)
    full = np.einsum("ghtj,qr->ghtqjr", outer, np.eye(keep))
    full = full.reshape(groups, groups, rows, each)
    tall = -(-rows // 8) * 8
    packed = np.zeros((groups, groups, 2 * tall, 2 * each))
    for half, places in enumerate(packing(each)):
        packed[:, :, half * tall : half * tall + rows, places] = full
    high, low = split(packed)
    image = np.concatenate([high, low], axis=2)
    inner = np.stack([right[:rank] for _, right, _ in parts])
    inner = inner.reshape(groups, rank, 2, bins_dev).transpose(0, 2, 1, 3)
    inner = np.repeat(inner, keep, axis=2)
    slot = -(-each // 8) * 8
    inner = np.pad(inner, ((0, 0), (0, 0), (0, slot - each), (0, 0)))
    return image, inner.reshape(groups, -1, bins_dev), each, slot


def body(
    cfg,
    series_hbm,
    kernel_hbm,
    prior_hbm,
    scale_hbm,
    short_hbm,
    tabs_hbm,
    img_hbm,
    out_ref,
    kbufs,
    rows,
    prior,
    scale,
    short,
    tabs,
    img_tab,
    inner,
    squeezed,
    arrived,
    spread,
    ebuf,
    left_mat,
    sbuf,
    rbuf,
    relay,
    joined,
    gath,
    lows,
    scaled,
    edges,
    halo_left,
    halo_right,
    small_sem,
    k_sem,
    g_send,
    g_recv,
    z_send,
    z_recv,
    relay_recv,
    x_send,
    x_recv,
    hl_send,
    hl_recv,
    hr_send,
    hr_recv,
    ready_x,
    ready_z,
    ready_far,
):
    groups, params, senses, chunks, joint, direct, bins_dev, probes, squeeze, each = cfg
    f = lax.axis_index("freq")
    k = lax.axis_index("param")
    s = lax.axis_index("sens")
    sens_dev = rows.shape[1]
    depth = kernel_hbm.shape[1]
    padded = left_mat.shape[1] // 2
    keep = probes // senses
    slot = inner.shape[1]
    width = 2 * LANES
    cols = scale.shape[1]
    count = len(chunks)
    has_left = k > 0
    has_right = k < params - 1
    has_under = s > 0
    has_over = s < senses - 1
    outer = jnp.logical_or(s == 0, s == senses - 1)
    within = jnp.logical_not(outer)
    second = lax.rem(k, 2) == 1
    first = jnp.logical_not(second)
    pair = s + 1 - 2 * lax.rem(s, 2)
    across = senses - 1 - s
    other = senses - 1 - pair

    def freq_peer(d):
        return lax.rem(f + d, groups)

    def tell(sem, **where):
        pl.semaphore_signal(sem, inc=1, device_id=where, device_id_type=MESH)

    small = [
        pltpu.make_async_copy(series_hbm, rows, small_sem.at[0]),
        pltpu.make_async_copy(short_hbm, short, small_sem.at[1]),
        pltpu.make_async_copy(tabs_hbm.at[f], tabs, small_sem.at[2]),
        pltpu.make_async_copy(prior_hbm, prior, small_sem.at[3]),
        pltpu.make_async_copy(scale_hbm, scale, small_sem.at[4]),
        pltpu.make_async_copy(img_hbm.at[f], img_tab, small_sem.at[5]),
    ]
    for copy in small:
        copy.start()

    barrier = pltpu.get_barrier_semaphore()
    for d in range(1, groups):
        tell(barrier, freq=freq_peer(d))

    @pl.when(has_under)
    def _():
        tell(barrier, sens=s - 1)

    @pl.when(has_over)
    def _():
        tell(barrier, sens=s + 1)

    @pl.when(has_left)
    def _():
        tell(barrier, param=k - 1)

    @pl.when(has_right)
    def _():
        tell(barrier, param=k + 1)

    row = lax.broadcasted_iota(jnp.int32, spread.shape, 0)
    lane = lax.broadcasted_iota(jnp.int32, spread.shape, 1)
    spread[...] = jnp.where(lane // bins_dev == row, 1.0, 0.0).astype(BF16)
    for buf in kbufs:
        pad = jnp.zeros((padded - depth, buf.shape[1]), BF16)
        buf[depth:padded] = pad
        buf[padded + depth :] = pad

    small[0].wait()
    small[1].wait()
    loads = [
        [
            pltpu.make_async_copy(
                kernel_hbm.at[part, :, pl.ds(chunks[c], width)],
                kbufs[i].at[pl.ds(part * padded, depth), pl.ds(n * width, width)],
                k_sem.at[i],
            )
            for n, c in enumerate(some)
            for part in range(2)
        ]
        for i, some in enumerate(joint)
    ]
    for group in loads:
        for copy in group:
            copy.start()

    series = rows[...]

    def shortened(g):
        both = jnp.dot(short[g], series, preferred_element_type=F32)
        return both[: squeeze * probes] + both[squeeze * probes :]

    main = sens_dev // LANES * LANES
    rest = sens_dev - main
    tall_rows = squeeze * probes
    fit = LANES // rest

    def fold(part):
        lines = [part[i : i + PAIR] for i in range(0, tall_rows, PAIR)]
        folded = []
        for i in range(0, len(lines), fit):
            some = lines[i : i + fit]
            gap = jnp.zeros((PAIR, LANES - rest * len(some)), F32)
            folded.append(jnp.concatenate(some + [gap], axis=1))
        return folded

    def unfold(packed):
        parts = []
        for i in range(tall_rows // PAIR):
            line = packed[i // fit * PAIR : (i // fit + 1) * PAIR]
            parts.append(line[:, i % fit * rest : (i % fit + 1) * rest])
        return jnp.concatenate(parts, axis=0)

    for d in range(1, groups):
        g = freq_peer(d)
        value = shortened(g)
        wide = [value[:, i : i + LANES] for i in range(0, main, LANES)]
        squeezed[g] = jnp.concatenate(wide + fold(value[:, main:]), axis=0).astype(BF16)

    beside = [has_under, has_over, has_left, has_right]
    pl.semaphore_wait(barrier, groups - 1 + sum(jnp.where(b, 1, 0) for b in beside))

    def series_copy(target, slot):
        return pltpu.make_async_remote_copy(
            src_ref=squeezed.at[target],
            dst_ref=arrived.at[slot],
            send_sem=g_send,
            recv_sem=g_recv,
            device_id={"freq": target},
            device_id_type=MESH,
        )

    for d in range(1, groups):
        series_copy(freq_peer(d), f).start()
    for d in range(1, groups):
        tell(ready_x, freq=freq_peer(d))

    @pl.when(within)
    def _():
        tell(ready_z, sens=s - 1)
        tell(ready_z, sens=s + 1)

    for copy in small[2:]:
        copy.wait()
    norm = 1.0 / math.sqrt(bins_dev * groups)
    lane = lax.broadcasted_iota(jnp.int32, (8, STEP), 1) % bins_dev
    value = jnp.zeros((8, STEP), F32)
    for b in range(bins_dev):
        value = jnp.where(lane == b, prior[b] * norm, value)
    base = groups * 2 * squeeze
    for q in range(2):
        inner[q] = tabs[base + q * slot : base + (q + 1) * slot] * value[:1]

    cuts = [(at, min(STEP, padded - at)) for at in range(0, padded, STEP)]

    def expand(parts, at, span):
        first = at // bins_dev // LANES
        rows_of = spread[first * LANES : min((first + 1) * LANES, sens_dev), at : at + span]
        return jnp.dot(parts[first], rows_of, preferred_element_type=F32)

    def weighed(full, d, q, span):
        total = None
        for j in range(squeeze):
            at = (d * 2 + q) * squeeze + j
            term = full[j * probes : (j + 1) * probes] * tabs[at : at + 1, :span]
            total = term if total is None else total + term
        return total

    mine = shortened(f)
    high = mine.astype(BF16)
    low = (mine - high.astype(F32)).astype(BF16)
    mine = jnp.concatenate([high, low], axis=0)
    mine_parts = [mine[:, i : min(i + LANES, sens_dev)] for i in range(0, sens_dev, LANES)]
    for at, span in cuts:
        full = expand(mine_parts, at, span)
        full = full[: squeeze * probes] + full[squeeze * probes :]
        for q in range(2):
            ebuf[q, :, at : at + span] = weighed(full, 0, q, span)

    pl.semaphore_wait(ready_z, 1)

    @pl.when(within)
    def _():
        tell(ready_far, sens=pair)

    def loaded(i):
        part = kbufs[i].at[pl.ds(0, 2 * depth)]
        pltpu.make_async_copy(part, part, k_sem.at[i]).wait()

    loaded(0)

    def series_done():
        return pltpu.make_async_remote_copy(
            src_ref=squeezed.at[pl.ds(0, groups - 1)],
            dst_ref=arrived.at[pl.ds(0, groups - 1)],
            send_sem=g_send,
            recv_sem=g_recv,
            device_id={"freq": freq_peer(1)},
            device_id_type=MESH,
        )

    @pl.when(within)
    def _():
        for c in range(count):
            if c not in direct:
                rbuf[other, c] = jnp.zeros(rbuf.shape[2:], BF16)

    series_done().wait_recv()
    came = []
    for d in range(1, groups):
        got = arrived.at[freq_peer(d)]
        parts = [got[i * tall_rows : (i + 1) * tall_rows] for i in range(main // LANES)]
        tail = got[main // LANES * tall_rows :].astype(F32)
        came.append(parts + [unfold(tail).astype(BF16)])
    head = None
    for group in [cuts[i : i + 2] for i in range(0, len(cuts), 2)]:
        for at, span in group:
            cut = slice(at, at + span)
            fulls = [expand(c, at, span) for c in came]
            for q in range(2):
                total = ebuf[q, :, cut]
                for d in range(1, groups):
                    total = total + weighed(fulls[d - 1], d, q, span)
                ebuf[q, :, cut] = total
            which = lax.broadcasted_iota(jnp.int32, (8, span), 0) % keep
            for j in range(senses):
                both = []
                for q in range(2):
                    e = jnp.broadcast_to(ebuf[q, j * keep : j * keep + 1, cut], (8, span))
                    for r in range(1, keep):
                        here = j * keep + r
                        e = jnp.where(which == r, ebuf[q, here : here + 1, cut], e)
                    both.append(jnp.concatenate([e] * (slot // 8), axis=0))
                re, im = both
                one, two = inner[0, :, :span], inner[1, :, :span]
                block = slice(j * slot, (j + 1) * slot)
                left_mat[block, cut] = (one * re + two * im).astype(BF16)
                left_mat[block, padded + at : padded + at + span] = (one * im - two * re).astype(BF16)
        start, stop = group[0][0], group[-1][0] + group[-1][1]
        for base in (0, padded):
            term = jnp.dot(
                left_mat[:, base + start : base + stop],
                kbufs[0][base + start : base + stop],
                preferred_element_type=F32,
            )
            head = term if head is None else head + term

    def remote(src, dst, send, recv, **where):
        return pltpu.make_async_remote_copy(
            src_ref=src,
            dst_ref=dst,
            send_sem=send,
            recv_sem=recv,
            device_id=where,
            device_id_type=MESH,
        )

    def z_copy(target, c):
        return remote(
            sbuf.at[target, c], rbuf.at[s, c], z_send, z_recv.at[c], sens=target
        )

    def z_done(units, c):
        part = rbuf.at[pl.ds(0, units), c]
        return remote(part, part, z_send, z_recv.at[c], sens=pair)

    def relay_copy(c):
        return remote(
            sbuf.at[other, c], relay.at[c], z_send, relay_recv.at[c], sens=pair
        )

    def joined_copy(c):
        return remote(
            joined.at[c], rbuf.at[s, c], z_send, z_recv.at[c], sens=across
        )

    def send_far(c):
        if c in direct:
            z_copy(across, c).start()
            if c == count - 1:
                z_copy(other, c).start()
                return

            @pl.when(within)
            def _():
                z_copy(other, c).start()

            return

        @pl.when(outer)
        def _():
            relay_copy(c).start()
            z_copy(across, c).start()

        @pl.when(within)
        def _():
            z_copy(other, c).start()

    def pass_on(c):
        if c in direct:
            return

        @pl.when(within)
        def _():
            relay_copy(c).wait_recv()
            both = sbuf[across, c].astype(F32) + relay[c].astype(F32)
            joined[c] = both.astype(BF16)
            joined_copy(c).start()

    def collect(c):
        if c in direct:
            z_done(3, c).wait_recv()
        else:

            @pl.when(outer)
            def _():
                z_done(3, c).wait_recv()

            @pl.when(within)
            def _():
                z_done(2, c).wait_recv()

        total = sbuf[s, c].astype(F32)
        for slot in (pair, other, across):
            total = total + rbuf[slot, c].astype(F32)
        return total

    whole = each // 8 * 8
    for i, some in enumerate(joint):
        total = head
        if i > 0:
            loaded(i)
            total = jnp.dot(left_mat[...], kbufs[i][...], preferred_element_type=F32)
        for n, c in enumerate(some):
            for j in range(senses):
                block = total[j * slot : (j + 1) * slot, n * width : (n + 1) * width]
                halves = [block[:, h * LANES : (h + 1) * LANES] for h in range(2)]
                packed = [half[:whole] for half in halves]
                if slot > each:
                    turned = pltpu.roll(halves[1][whole:], each - whole, 0)
                    packed.append(halves[0][whole:] + turned)
                sbuf[j, c] = jnp.concatenate(packed, axis=0).astype(BF16)
        if i == 0:

            @pl.when(outer)
            def _():
                pl.semaphore_wait(ready_far, 1)

        for c in some:
            send_far(c)
        if i == 0 or i == len(joint) - 1:
            late = [c for part in joint[min(i, 1) : i + 1] for c in part]
            for c in late:
                if c in direct and c < count - 1:
                    pl.when(outer)(z_copy(other, c).start)
            for c in late:
                z_copy(pair, c).start()

    def x_copy(target, c):
        part = gath.at[f, c]
        return remote(part, part, x_send, x_recv.at[c], freq=target)

    def x_done(c):
        part = gath.at[pl.ds(0, groups - 1), c]
        return remote(part, part, x_send, x_recv.at[c], freq=freq_peer(1))

    def to_left(target):
        return remote(
            edges.at[0],
            halo_right.at[f],
            hl_send,
            hr_recv,
            freq=target,
            param=jnp.maximum(k - 1, 0),
        )

    def to_right(target):
        return remote(
            edges.at[1],
            halo_left.at[f],
            hr_send,
            hl_recv,
            freq=target,
            param=jnp.minimum(k + 1, params - 1),
        )

    rows_out = scaled.shape[0]
    tall = img_tab.shape[1] // 4

    def image_of(pieces, lower=None):
        total = None
        for g, piece in pieces:
            term = jnp.dot(img_tab[g], piece, preferred_element_type=F32)
            total = term if total is None else total + term
        total = total[: 2 * tall] + total[2 * tall :]
        if lower is not None:
            total = total + jnp.dot(img_tab[f, : 2 * tall], lower, preferred_element_type=F32)
        return total[:rows_out], total[tall : tall + rows_out]

    def begin(c):
        for half, image in enumerate(image_of([(f, gath[f, c])], lows[c])):
            at = chunks[c] + half * LANES
            scaled[:, at : at + LANES] = image

    def finish(c):
        x_done(c).wait_recv()
        pieces = [(freq_peer(d), gath[freq_peer(d), c]) for d in range(1, groups)]
        for half, image in enumerate(image_of(pieces)):
            at = chunks[c] + half * LANES
            lanes = slice(at, at + LANES)
            scaled[:, lanes] = (scaled[:, lanes] + image) * scale[:, lanes]

    pl.semaphore_wait(ready_x, groups - 1)
    for c in range(count):
        pass_on(c)
    for c, at in enumerate(chunks):
        total = collect(c)
        high = total.astype(BF16)
        gath[f, c] = high
        for d in range(1, groups):
            x_copy(freq_peer(d), c).start()
        lows[c] = (total - high.astype(F32)).astype(BF16)
        if at == 0:
            edges[0] = (total * scale[:, :LANES]).astype(BF16)

            @pl.when(has_left)
            def _():
                for d in range(groups):
                    to_left(freq_peer(d)).start()

        if at + width == cols:
            edges[1] = (total * scale[:, cols - LANES :]).astype(BF16)

            @pl.when(has_right)
            def _():
                for d in range(groups):
                    to_right(freq_peer(d)).start()

    for c in range(count):
        begin(c)

    def halo_done(ref, send, recv):
        return remote(ref, ref, send, recv, freq=freq_peer(1))

    @pl.when(has_left)
    def _():
        halo_done(halo_left, hr_send, hl_recv).wait_recv()

    @pl.when(jnp.logical_not(has_left))
    def _():
        halo_left[...] = jnp.zeros_like(halo_left)

    @pl.when(has_right)
    def _():
        halo_done(halo_right, hl_send, hr_recv).wait_recv()

    @pl.when(jnp.logical_not(has_right))
    def _():
        halo_right[...] = jnp.zeros_like(halo_right)

    _, left = image_of([(g, halo_left[g]) for g in range(groups)])
    right, _ = image_of([(g, halo_right[g]) for g in range(groups)])
    for c in range(count - 1):
        finish(c)

    def smooth(at, end):
        if at >= end:
            return
        mid = scaled[:, at:end]
        before = scaled[:, at - 1 : at] if at > 0 else left[:, LANES - 1 :]
        after = scaled[:, end : end + 1] if end < cols else right[:, :1]
        lower = jnp.concatenate([before, mid[:, :-1]], axis=1)
        upper = jnp.concatenate([mid[:, 1:], after], axis=1)
        value = scale[:, at:end] * (0.5 * mid + 0.25 * (lower + upper))
        out_ref[:, :, at:end] = value.reshape(out_ref.shape[0], keep, end - at)

    at = chunks[-1]
    start, stop = max(at - LANES, 0), min(at + width + LANES, cols)
    smooth(0, start)
    smooth(stop, cols)
    finish(count - 1)
    smooth(start, stop)

    series_done().wait_send()
    part = sbuf.at[pl.ds(0, 3)]
    remote(part, part, z_send, z_recv.at[0], sens=pair).wait_send()
    part = gath.at[pl.ds(0, groups - 1)]
    remote(part, part, x_send, x_recv.at[0], freq=freq_peer(1)).wait_send()

    @pl.when(has_left)
    def _():
        halo_done(halo_right, hl_send, hr_recv).wait_send()

    @pl.when(has_right)
    def _():
        halo_done(halo_left, hr_send, hl_recv).wait_send()


def local(mesh_shape, series, kernel, prior_spectrum, prior_scale):
    groups, params, senses = (mesh_shape[n] for n in ("freq", "param", "sens"))
    assert senses == 4 and groups > 1
    probes, sens_dev, time_dev = series.shape
    _, bins_dev, _, cols = kernel.shape
    keep = probes // senses
    width = 2 * LANES
    assert cols % width == 0
    chunks = list(range(0, cols, width))
    chunks = chunks[:1] + chunks[:0:-1][:1] + chunks[1:-1]
    direct = tuple(range(len(chunks) // 2, len(chunks)))
    joint = [[0], list(range(1, len(chunks) - 1)), [len(chunks) - 1]]
    count = len(chunks)
    depth = sens_dev * bins_dev
    padded = -(-depth // LANES) * LANES
    short, long, squeeze = series_tables(groups, bins_dev, time_dev, probes)
    img_tab, inner, each, slot = image_tables(groups, bins_dev, time_dev, keep)
    tabs = np.concatenate([long, inner], axis=1)
    main = sens_dev // LANES
    fit = LANES // (sens_dev - main * LANES)
    assert squeeze * probes % PAIR == 0
    lines = main * squeeze * probes + -(-squeeze * probes // PAIR // fit) * PAIR
    tabs = np.tile(tabs, (1, 1, STEP // bins_dev)).astype(np.float32)
    unit = (2 * each, LANES)
    dma = pltpu.SemaphoreType.DMA
    plain = pltpu.SemaphoreType.REGULAR
    return pl.pallas_call(
        functools.partial(
            body, (groups, params, senses, chunks, joint, direct, bins_dev, probes, squeeze, each)
        ),
        out_shape=pltpu.VMEM((time_dev, keep, cols), F32),
        in_specs=[pl.BlockSpec(memory_space=pltpu.HBM)] * 7,
        out_specs=pl.BlockSpec(memory_space=pltpu.VMEM),
        scratch_shapes=[
            [pltpu.VMEM((2 * padded, width * len(some)), BF16) for some in joint],
            pltpu.VMEM((time_dev * probes, sens_dev), BF16),
            pltpu.SMEM((bins_dev,), F32),
            pltpu.VMEM((1, cols), F32),
            pltpu.VMEM(short.shape, BF16),
            pltpu.VMEM(tabs.shape[1:], F32),
            pltpu.VMEM(img_tab.shape[1:], BF16),
            pltpu.VMEM((2, slot, STEP), F32),
            pltpu.VMEM((groups, lines, LANES), BF16),
            pltpu.VMEM((groups, lines, LANES), BF16),
            pltpu.VMEM((sens_dev, padded), BF16),
            pltpu.VMEM((2, probes, padded), F32),
            pltpu.VMEM((senses * slot, 2 * padded), BF16),
            pltpu.VMEM((senses, count) + unit, BF16),
            pltpu.VMEM((senses, count) + unit, BF16),
            pltpu.VMEM((count,) + unit, BF16),
            pltpu.VMEM((count,) + unit, BF16),
            pltpu.VMEM((groups, count) + unit, BF16),
            pltpu.VMEM((count,) + unit, BF16),
            pltpu.VMEM((time_dev * keep, cols), F32),
            pltpu.VMEM((2,) + unit, BF16),
            pltpu.VMEM((groups,) + unit, BF16),
            pltpu.VMEM((groups,) + unit, BF16),
            dma((6,)),
            dma((len(joint),)),
            dma,
            dma,
            dma,
            dma((count,)),
            dma((count - len(direct),)),
            dma,
            dma((count,)),
            dma,
            dma,
            dma,
            dma,
            plain,
            plain,
            plain,
        ],
        compiler_params=pltpu.CompilerParams(
            collective_id=0, has_side_effects=True, vmem_limit_bytes=60 * 1024 * 1024
        ),
    )(
        series.transpose(2, 0, 1).reshape(time_dev * probes, sens_dev),
        kernel.transpose(0, 2, 1, 3).reshape(2, depth, cols),
        prior_spectrum,
        prior_scale.reshape(1, cols),
        jnp.asarray(short),
        jnp.asarray(tabs),
        jnp.asarray(img_tab),
    )


def solution(mesh):
    placed = (P(None, "sens", "freq"), P(None, "freq", "sens", "param"), P("freq"), P("param"))
    return jax.shard_map(
        functools.partial(local, dict(mesh.shape)),
        mesh=mesh,
        in_specs=placed,
        out_specs=P("freq", "sens", "param"),
        check_vma=False,
    )
```
